128 devices in a mesh: seq: 16 (over z, y), mp: 8 (over x, core).
Axes of the slice: x: 4, y: 4, z: 4, core: 2. Of those that a mesh axis runs over, the one named last changes fastest.
Arguments:
- resid: bfloat16 [4096, 5120], P('seq', 'mp'), may hold values from -15 to 15
- queries: bfloat16 [4096, 5120], P('seq', 'mp'), may hold values from -28 to 28
- keys: bfloat16 [4096, 5120], P('seq', 'mp'), may hold values from -12.25 to 12.25
- values: bfloat16 [4096, 5120], P('seq', 'mp'), may hold values from -6 to 6
- doc_ids: int32 [4096], P('seq'), may hold values from 0 to 3, as said below
- out_proj: bfloat16 [5120, 5120], P('mp'), may hold values from -0.5 to 0.5
- ffn_gain: bfloat16 [5120], P('mp'), may hold values from 0.25 to 1.75
- w_in: bfloat16 [5120, 13824], P('mp', 'seq'), may hold values from -0.078125 to 0.078125
- w_out: bfloat16 [13824, 5120], P('seq', 'mp'), may hold values from -0.109375 to 0.109375
- hot_index: int32 [16, 384], P('seq'), may hold values from 0 to 863, as said below
- hot_blocks: int32 [16], P('seq'), may hold values from 1 to 3, as said below
Outputs:
- layer_out: bfloat16 [4096, 5120], P('seq', 'mp')
- hot_mean: float32 [16, 384], P('seq')
The draws below stay inside these ranges and needn't reach their ends.
Inputs may be any that keep to these rules, and one draw needn't show every extreme that they name: `doc_ids`: document numbers never fall along the tokens; every number from 0 to 3 occurs; some document has 2048 tokens. `hot_index`: row g holds 384 distinct neuron numbers of group g; only its first 128 * hot_blocks[g] entries are live, the others are ignored. `hot_blocks`: some group has exactly 3 live blocks.
All inputs are finite; a program needn't handle non-finite values.
Results may differ from the reference program's by a relative error of at most 0.014.
Values may be sent and summed in bfloat16 or wider, within the bound.
A program may use at most 192 MiB of HBM per device.

```python
import jax
import jax.numpy as jnp
from jax import lax

D = 5120
HEADS = 40
HEAD_DIM = 128
FF = 13824
BLOCK = 128
CAP = 3
TOKENS = 4096
GROUPS = 16
NEURONS = 864
SLOTS = 384


def paired_rows(key, which):
    noise = jnp.clip(jax.random.normal(jax.random.fold_in(key, 101 + which), (TOKENS, D), jnp.float32), -4.0, 4.0)
    return noise


def draw_resid(key, part):
    ramp = jnp.arange(D, dtype=jnp.float32) / (D - 1)
    rough = jnp.exp(jax.random.uniform(jax.random.fold_in(key, 501), (D,), jnp.float32, jnp.log(0.7), jnp.log(1.4)))
    column_scale = 0.5 * jnp.exp(ramp * jnp.log(5.0)) * rough
    noise = jnp.clip(jax.random.normal(jax.random.fold_in(key, 504), (TOKENS, D), jnp.float32), -4.0, 4.0)
    return (noise * column_scale[None, :]).astype(jnp.bfloat16)


def draw_queries(key, part):
    return paired_rows(key, 0).astype(jnp.bfloat16)


def draw_keys(key, part):
    return paired_rows(key, 1).astype(jnp.bfloat16)


def draw_doc_ids(key, part):
    half = TOKENS // 2
    cut_one = jax.random.randint(jax.random.fold_in(key, 401), (), 1, half - 1)
    cut_two = cut_one + half
    cut_three = jax.random.randint(jax.random.fold_in(key, 402), (), cut_two + 1, TOKENS)
    places = jnp.arange(TOKENS, dtype=jnp.int32)
    marks = (places >= cut_one).astype(jnp.int32) + (places >= cut_two).astype(jnp.int32) + (places >= cut_three).astype(jnp.int32)
    return marks.astype(jnp.int32)


def draw_hot_index(key, part):
    group_keys = jax.random.split(jax.random.fold_in(key, 201), GROUPS)
    orders = jax.vmap(lambda single: jax.random.permutation(single, NEURONS))(group_keys)
    return orders[:, :SLOTS].astype(jnp.int32)


def draw_hot_blocks(key, part):
    busy = jax.random.randint(jax.random.fold_in(key, 301), (GROUPS,), 0, 3) == 0
    extra = jax.random.randint(jax.random.fold_in(key, 302), (GROUPS,), 2, CAP + 1)
    counts = jnp.where(busy, extra, 1)
    heaviest = jax.random.randint(jax.random.fold_in(key, 303), (), 0, GROUPS)
    return jnp.where(jnp.arange(GROUPS) == heaviest, CAP, counts).astype(jnp.int32)


def block_levels(stream_key, shape, cuts, least, largest):
    level = 1.0
    for position, parts in cuts:
        steps = jax.random.uniform(jax.random.fold_in(jax.random.fold_in(stream_key, 6), position), (parts,), jnp.float32, least / len(cuts), largest / len(cuts))
        level = level * jnp.repeat(jnp.exp(steps), shape[position] // parts).reshape((-1,) + (1,) * (len(shape) - 1 - position))
    return level


def bell_draw(stream_key, shape, deviation, bound, shards=(), kind=jnp.bfloat16):
    factor_of = block_levels(stream_key, shape, shards, -0.22, 0.18) if shards else 1.0
    values = jax.random.normal(stream_key, shape, jnp.float32) * deviation * factor_of
    return jnp.minimum(jnp.maximum(values, -bound), bound).astype(kind)


def setup_inputs(seed: int = 0) -> dict:
    splits = jax.random.split(jax.random.key(seed), 12)
    return {
        "resid": draw_resid(jax.random.fold_in(splits[11], 71), 0),
        "queries": draw_queries(jax.random.fold_in(splits[11], 71), 0),
        "keys": draw_keys(jax.random.fold_in(splits[11], 71), 0),
        "values": bell_draw(splits[3], (TOKENS, D), 1.0, 6.0, ((0, 16), (1, 8))),
        "doc_ids": draw_doc_ids(jax.random.fold_in(splits[11], 71), 0),
        "out_proj": bell_draw(splits[5], (D, D), HEAD_DIM ** -0.5, 0.5, ((0, 8),)),
        "ffn_gain": jnp.clip(1.0 + 0.15 * jax.random.normal(splits[6], (D,), jnp.float32), 0.25, 1.75).astype(jnp.bfloat16),
        "w_in": bell_draw(splits[7], (D, FF), D ** -0.5, 0.078125, ((0, 8), (1, 16))),
        "w_out": bell_draw(splits[8], (FF, D), (FF // 4) ** -0.5, 0.109375, ((0, 16), (1, 8))),
        "hot_index": draw_hot_index(jax.random.fold_in(splits[11], 71), 0),
        "hot_blocks": draw_hot_blocks(jax.random.fold_in(splits[11], 71), 0),
    }


epsilon = 1e-05
masked_score = -1e+30

def reference(resid, queries, keys, values, doc_ids, out_proj, ffn_gain, w_in, w_out, hot_index, hot_blocks):
    scale = HEAD_DIM ** (-0.5)
    positions = jnp.arange(TOKENS, dtype=jnp.int32)
    visible = (positions[:, None] >= positions[None, :]) & (doc_ids[:, None] == doc_ids[None, :])

    def one_head(triple):
        query_head, key_head, value_head = triple
        scores = jnp.dot(query_head, key_head.T, preferred_element_type=jnp.float32) * scale
        scores = jnp.where(visible, scores, masked_score)
        top = lax.optimization_barrier(jnp.max(scores, axis=1, keepdims=True))
        weights = jnp.where(visible, jnp.exp(scores - top), 0.0)
        total = lax.optimization_barrier(jnp.sum(weights, axis=1, keepdims=True))
        mixed = jnp.dot(weights.astype(jnp.bfloat16), value_head, preferred_element_type=jnp.float32)
        return (mixed / total).astype(jnp.bfloat16)
    split_queries = queries.reshape(TOKENS, HEADS, HEAD_DIM).transpose(1, 0, 2)
    split_keys = keys.reshape(TOKENS, HEADS, HEAD_DIM).transpose(1, 0, 2)
    split_values = values.reshape(TOKENS, HEADS, HEAD_DIM).transpose(1, 0, 2)
    attended = lax.map(one_head, (split_queries, split_keys, split_values))
    attended = attended.transpose(1, 0, 2).reshape(TOKENS, D)
    projected = jnp.dot(attended, out_proj, preferred_element_type=jnp.float32)
    state_rows = (resid.astype(jnp.float32) + projected).astype(jnp.bfloat16)
    widened = state_rows.astype(jnp.float32)
    inverse = lax.rsqrt(lax.optimization_barrier(jnp.mean(widened * widened, axis=1, keepdims=True)) + epsilon)
    normed = (widened * inverse * ffn_gain.astype(jnp.float32)).astype(jnp.bfloat16)
    slot_ids = jnp.arange(SLOTS, dtype=jnp.int32)

    def one_group(carry, group):
        columns = (group * NEURONS + hot_index[group]).astype(jnp.int32)
        live = slot_ids < BLOCK * hot_blocks[group]
        before = jnp.dot(normed, jnp.take(w_in, columns, axis=1), preferred_element_type=jnp.float32)
        active = jnp.where(live[None, :], jnp.maximum(before, 0.0), 0.0)
        carry = carry + jnp.dot(active.astype(jnp.bfloat16), jnp.take(w_out, columns, axis=0), preferred_element_type=jnp.float32)
        return (carry, lax.optimization_barrier(jnp.mean(active, axis=0)))
    ffn_sum, hot_mean = lax.scan(one_group, jnp.zeros((TOKENS, D), jnp.float32), jnp.arange(GROUPS, dtype=jnp.int32))
    layer_out = (widened + ffn_sum).astype(jnp.bfloat16)
    return (layer_out, hot_mean)
```

```python
import jax
import jax.numpy as jnp
from jax import lax
from jax.experimental import pallas as pl
from jax.experimental.pallas import tpu as pltpu
from jax.sharding import PartitionSpec as P

HEAD_DIM = 128
HEADS = 5
TOK = 256
WID = 640
SLOTS = 384
BLOCK = 128
NEUR = 864
D = 5120
TOKENS = 4096
EPS = 1e-05
LOW = -1e9
MASKED = -2e9
SCALE2 = HEAD_DIM ** (-0.5) * 1.4426950408889634
BF = jnp.bfloat16
F32 = jnp.float32
ORDER = (1, 3, 2)


def dot(a, b, dims):
    return lax.dot_general(a, b, (dims, ((), ())), preferred_element_type=F32)


def kernel(
    q_ref, k_ref, v_ref, resid_ref, doc_ref, oproj_ref, gain_ref, win_ref, wout_ref, hidx_ref,
    hblk_ref, out_ref, hm_ref,
    qb, kb, vb, drow, qrow, kcol, accw, acc0, st0, osend, ssend, orecv, srecv, att, wo, res,
    psend, precv, wi_own, wo_own, hin, win, wou, sqs, nb, prebuf, presend, prerecv, ab, fown,
    fsend, frecv, csum, csr, hs, hsr,
    kv_s, kv_r, q_s, q_r, d_s, d_r, o_s, o_r, a_s, a_r, wo_s, wo_r, wo_l, p_s, p_r, l_s, own_l,
    wi_s, wi_r, wu_s, wu_r, sq_s, sq_r, n_s, n_r, nd_s, nd_r, rs_s, rs_r, ag_s, ag_r, ad_s, ad_r,
    f_s, f_r, c_s, c_r, h_s, h_r,
):
    s = lax.axis_index("seq")
    m = lax.axis_index("mp")
    z, y, x, c = s // 4, s % 4, m // 2, m % 2

    def dev(dz=0, dy=0, dx=0, dc=0):
        return (((z + dz) % 4) * 4 + (y + dy) % 4, ((x + dx) % 4) * 2 + (c + dc) % 2)

    def remote(src, dst, ss, rs, device):
        return pltpu.make_async_remote_copy(
            src_ref=src, dst_ref=dst, send_sem=ss, recv_sem=rs, device_id=device,
            device_id_type=pl.DeviceIdType.MESH,
        )

    peer = dev(dc=1)
    sent = []

    def go(cp):
        cp.start()
        sent.append(cp)
        return cp

    def lane(ref, h):
        return ref.at[:, h * HEAD_DIM : (h + 1) * HEAD_DIM]

    loads = []
    for h in range(HEADS):
        for j, (src, dst) in enumerate(((q_ref, qb), (k_ref, kb), (v_ref, vb))):
            cp = pltpu.make_async_copy(lane(src, h), dst.at[0, h], own_l.at[j, h])
            cp.start()
            loads.append(cp)
    big = [
        pltpu.make_async_copy(win_ref, wi_own, l_s.at[0]),
        pltpu.make_async_copy(wout_ref, wo_own, l_s.at[1]),
        pltpu.make_async_copy(resid_ref, res, l_s.at[2]),
    ]
    for cp in big:
        cp.start()

    barrier = pltpu.get_barrier_semaphore()
    friends = [peer]
    for r in (1, 2, 3):
        friends += [dev(dy=r), dev(dy=r, dc=1), dev(dz=r), dev(dx=r), dev(dx=r, dc=1)]
    for f in friends:
        pl.semaphore_signal(barrier, inc=1, device_id=f, device_id_type=pl.DeviceIdType.MESH)
    doc_here = jnp.broadcast_to(doc_ref[...].astype(F32), (8, TOK))
    drow[0] = doc_here
    qrow[0] = doc_here
    pl.semaphore_wait(barrier, len(friends))

    doc_in = []
    for r in (1, 2, 3):
        doc_in.append(go(remote(drow.at[0], drow.at[r], d_s.at[r], d_r.at[r], dev(dy=r))))
    for r in (1, 2):
        doc_in.append(go(remote(drow.at[0], qrow.at[r], d_s.at[3 + r], d_r.at[3 + r], dev(dz=-r))))
    for h in range(HEADS):
        for r in ORDER:
            go(remote(lane(k_ref, h), kb.at[r, h], kv_s.at[0, r, h], kv_r.at[0, r, h], dev(dy=r)))
            go(remote(lane(v_ref, h), vb.at[r, h], kv_s.at[1, r, h], kv_r.at[1, r, h], dev(dy=r)))
        for r in (1, 2):
            go(remote(lane(q_ref, h), qb.at[r, h], q_s.at[r, h], q_r.at[r, h], dev(dz=-r)))

    wo_loc, wo_rem = [], []
    rows_c = pl.ds(pl.multiple_of(c * WID, 128), WID)
    for d in range(4):
        mine = pl.ds(pl.multiple_of((2 * d + c) * WID, 128), WID)
        theirs = pl.ds(pl.multiple_of((2 * d + 1 - c) * WID, 128), WID)
        cp = pltpu.make_async_copy(oproj_ref.at[:, mine], wo.at[d, rows_c, :], wo_l.at[d])
        cp.start()
        wo_loc.append(cp)
        wo_rem.append(
            go(remote(oproj_ref.at[:, theirs], wo.at[d, rows_c, :], wo_s.at[d], wo_r.at[d], peer))
        )

    for cp in big:
        cp.wait()
    live = lax.broadcasted_iota(jnp.int32, (1, SLOTS), 1) < BLOCK * hblk_ref[0]
    want = jnp.where(live, hidx_ref[...], -1)
    pick = (lax.broadcasted_iota(jnp.int32, (NEUR, SLOTS), 0) == want).astype(F32).astype(BF)
    hin[...] = dot(wi_own[...], pick, ((1,), (0,))).astype(BF)
    my_rows = pl.ds(pl.multiple_of(y * SLOTS, 128), SLOTS)
    wou[my_rows, :] = dot(pick, wo_own[...], ((0,), (0,))).astype(BF)
    ct = y // 2
    win_dst = win.at[rows_c, pl.ds(pl.multiple_of((y % 2) * SLOTS, 128), SLOTS)]

    @pl.when(ct == c)
    def _():
        win[rows_c, pl.ds(pl.multiple_of((y % 2) * SLOTS, 128), SLOTS)] = hin[...]

    wi_peer = remote(hin, win_dst, wi_s.at[0], wi_r.at[y % 2, c], peer)

    @pl.when(ct != c)
    def _():
        wi_peer.start()

    wu_in = []
    for r in ORDER:
        go(
            remote(
                hin, win_dst, wi_s.at[r], wi_r.at[y % 2, c],
                (z * 4 + (y + r) % 4, 2 * x + ct),
            )
        )
        wu_in.append(
            go(remote(wou.at[my_rows], wou.at[my_rows], wu_s.at[r], wu_r.at[r], dev(dy=r)))
        )

    for cp in loads:
        cp.wait()
    for cp in doc_in:
        cp.wait_recv()
    for r in range(4):
        kcol[r] = jnp.transpose(jnp.broadcast_to(drow[r][0:1, :], (128, TOK)))

    def step(h, i, r, qd, top, total, causal):
        sc = dot(kb[r, h], qb[i, h], ((1,), (1,)))
        kd = kcol[r]
        mask = jnp.concatenate([kd, kd], axis=1) == qd
        if causal:
            key_at = lax.broadcasted_iota(jnp.int32, (TOK, TOK), 0)
            query_at = lax.broadcasted_iota(jnp.int32, (TOK, TOK), 1)
            mask = mask & (key_at <= query_at)
        sc = jnp.where(mask, sc, MASKED)
        new = jnp.maximum(top, jnp.max(sc, axis=0, keepdims=True))
        p = jnp.exp2((sc - new) * SCALE2)
        fade = jnp.exp2((top - new) * SCALE2)
        total = total * fade + jnp.sum(p, axis=0, keepdims=True)
        accw[...] = accw[...] * fade + dot(vb[r, h], p.astype(BF), ((0,), (0,)))
        return new, total

    low = jnp.full((1, TOK), LOW, F32)
    zero = jnp.zeros((1, TOK), F32)

    def both(top, total):
        row = lax.broadcasted_iota(jnp.int32, (8, TOK), 0)
        return jnp.where(row == 0, top, total)

    def back(i, h):
        return (
            remote(
                osend.at[i - 1, h], orecv.at[i - 1, h], o_s.at[0, i - 1, h], o_r.at[0, i - 1, h],
                (((z + i) % 4) * 4 + y, m),
            ),
            remote(
                ssend.at[i - 1, h], srecv.at[i - 1, h], o_s.at[1, i - 1, h], o_r.at[1, i - 1, h],
                (((z + i) % 4) * 4 + y, m),
            ),
        )

    def head(h, _):
        for r in (1, 2):
            remote(qb.at[0, h], qb.at[r, h], q_s.at[r, h], q_r.at[r, h], dev(dz=-r)).wait_recv()
        for r in ORDER:
            remote(kb.at[0, h], kb.at[r, h], kv_s.at[0, r, h], kv_r.at[0, r, h], peer).wait_recv()
            remote(vb.at[0, h], vb.at[r, h], kv_s.at[1, r, h], kv_r.at[1, r, h], peer).wait_recv()

        def away(t, _):
            i = 2 - t
            qd = jnp.where(z + i <= 3, qrow[i][0:1, :], -5.0)
            accw[...] = jnp.zeros_like(accw)

            def visit(n, carry):
                r = jnp.where(jnp.logical_and(i == 2, n > 0), y + n, n)
                return step(h, i, r, qd, *carry, False)

            top, total = lax.fori_loop(0, jnp.where(i == 2, 4 - y, 4), visit, (low, zero))
            osend[i - 1, h] = accw[...].astype(BF)
            ssend[i - 1, h] = both(top, total)
            for cp in back(i, h):
                cp.start()
            return 0

        lax.fori_loop(0, 2, away, 0)
        accw[...] = jnp.zeros_like(accw)
        qd = qrow[0][0:1, :]
        carry = step(h, 0, 0, qd, low, zero, True)
        top, total = lax.fori_loop(
            1, y + 1, lambda r, carry: step(h, 0, r, qd, *carry, False), carry
        )
        acc0[h] = accw[...]
        st0[h] = both(top, total)
        return 0

    lax.fori_loop(0, HEADS, head, 0)

    def swap(h):
        return remote(att.at[c, h], att.at[c, h], a_s.at[h], a_r.at[h], peer)

    def merge(h, _):
        for i in (1, 2):
            for cp in back(i, h):
                cp.wait_recv()
        t0, t1, t2 = st0[h][0:1, :], srecv[0, h][0:1, :], srecv[1, h][0:1, :]
        n0, n1, n2 = st0[h][1:2, :], srecv[0, h][1:2, :], srecv[1, h][1:2, :]
        top = jnp.maximum(t0, jnp.maximum(t1, t2))
        f0 = jnp.exp2((t0 - top) * SCALE2)
        f1 = jnp.exp2((t1 - top) * SCALE2)
        f2 = jnp.exp2((t2 - top) * SCALE2)
        inv = 1.0 / (n0 * f0 + n1 * f1 + n2 * f2)
        mixed = (
            acc0[h] * (f0 * inv)
            + orecv[0, h].astype(F32) * (f1 * inv)
            + orecv[1, h].astype(F32) * (f2 * inv)
        )
        att[c, h] = jnp.transpose(mixed).astype(BF)
        swap(h).start()
        return 0

    lax.fori_loop(0, HEADS, merge, 0)

    for cp in wo_loc:
        cp.wait()
    for cp in wo_rem:
        cp.wait_recv()
    for h in range(HEADS):
        remote(att.at[1 - c, h], att.at[1 - c, h], a_s.at[h], a_r.at[h], peer).wait_recv()
    both_att = jnp.concatenate([att[i, h] for i in (0, 1) for h in range(HEADS)], axis=1)
    p_in = []
    for r in (2, 1, 3):
        psend[r] = dot(both_att, wo[(x + r) % 4], ((1,), (0,))).astype(BF)
        p_in.append(go(remote(psend.at[r], precv.at[r], p_s.at[r], p_r.at[r], dev(dx=r))))
    fown[...] = dot(both_att, wo[x], ((1,), (0,))) + res[...].astype(F32)
    for cp in p_in:
        cp.wait_recv()
    state = (
        fown[...] + precv[1].astype(F32) + precv[2].astype(F32) + precv[3].astype(F32)
    ).astype(BF)
    res[...] = state

    wide = state.astype(F32)
    square = wide * wide
    high = square.astype(BF)
    rest = (square - high.astype(F32)).astype(BF)
    ones = jnp.ones((8, WID), BF)
    sqs[0] = dot(ones, high, ((1,), (1,))) + dot(ones, rest, ((1,), (1,)))
    sq_in = []
    for j in range(1, 8):
        cp = remote(
            sqs.at[0], sqs.at[j], sq_s.at[j], sq_r.at[j], dev(dx=j // 2, dc=j % 2)
        )
        sq_in.append(go(cp))
    for cp in sq_in:
        cp.wait_recv()
    squares = sqs[0]
    for j in range(1, 8):
        squares = squares + sqs[j]
    inverse = lax.rsqrt(squares[0:1, :] / D + EPS)
    column = jnp.transpose(jnp.broadcast_to(inverse, (128, TOK)))
    column = jnp.concatenate([column] * HEADS, axis=1)
    gain = gain_ref[...].astype(F32)
    nb[0, c] = (res[...].astype(F32) * column * gain).astype(BF)

    n_in = {}
    nd_in = {}
    nd_in[0] = go(remote(nb.at[0, c], nb.at[0, c], nd_s.at[0], nd_r.at[0], peer))
    for r in ORDER:
        n_in[r] = go(remote(nb.at[0, c], nb.at[r, c], n_s.at[r], n_r.at[r], dev(dz=r)))

    for cp in wu_in:
        cp.wait_recv()
    for gi in (0, 1):
        for cs in (0, 1):
            @pl.when(jnp.logical_not(jnp.logical_and(y == 2 * c + gi, c == cs)))
            def _():
                remote(hin, win_dst, wi_s.at[0], wi_r.at[gi, cs], peer).wait_recv()

    csum[...] = jnp.zeros_like(csum)
    rs_in, ag_in, ad_in, f_in = {}, {}, {}, {}
    my64 = pl.ds(pl.multiple_of(x * 64, 64), 64)

    def stage_a(r):
        if r:
            n_in[r].wait_recv()
            nd_in[r] = go(remote(nb.at[r, c], nb.at[r, c], nd_s.at[r], nd_r.at[r], peer))

    def stage_b(r):
        nd_in[r].wait_recv()
        rows = jnp.concatenate([nb[r, 0], nb[r, 1]], axis=1)
        pre = dot(rows, win[...], ((1,), (0,)))
        prebuf[r] = pre
        presend[r] = pre.astype(BF)
        for e in (2, 1, 3):
            there = pl.ds(pl.multiple_of(((x + e) % 4) * 64, 64), 64)
            rs_in[r, e] = go(
                remote(
                    presend.at[r, there], prerecv.at[r, e], rs_s.at[r, e], rs_r.at[r, e],
                    dev(dx=e),
                )
            )

    def stage_c(r):
        for e in (1, 3, 2):
            rs_in[r, e].wait_recv()
        pre = (
            prebuf[r, my64, :] + prerecv[r, 1].astype(F32) + prerecv[r, 2].astype(F32)
            + prerecv[r, 3].astype(F32)
        )
        active = jnp.maximum(pre, 0.0)
        csum[...] += jnp.sum(active, axis=0, keepdims=True)
        ab[r, c, my64, :] = active.astype(BF)
        for e in (2, 1, 3):
            ag_in[r, e] = go(
                remote(
                    ab.at[r, c, my64], ab.at[r, c, my64], ag_s.at[r, e], ag_r.at[r, e], dev(dx=e)
                )
            )

    def stage_d(r):
        for e in (1, 3, 2):
            ag_in[r, e].wait_recv()
        ad_in[r] = go(remote(ab.at[r, c], ab.at[r, c], ad_s.at[r], ad_r.at[r], peer))

    def stage_e(r):
        ad_in[r].wait_recv()
        rows = jnp.concatenate([ab[r, 0], ab[r, 1]], axis=1)
        part = dot(rows, wou[...], ((1,), (0,)))
        if r == 0:
            fown[...] = part
        else:
            fsend[r] = part.astype(BF)
            f_in[r] = go(remote(fsend.at[r], frecv.at[r], f_s.at[r], f_r.at[r], dev(dz=-r)))

    plan = (
        (stage_a, 0), (stage_b, 0), (stage_a, 1), (stage_b, 1), (stage_c, 0), (stage_a, 3),
        (stage_b, 3), (stage_c, 1), (stage_d, 0), (stage_a, 2), (stage_b, 2), (stage_c, 3),
        (stage_d, 1), (stage_e, 0), (stage_c, 2), (stage_d, 3), (stage_e, 1), (stage_d, 2),
        (stage_e, 3), (stage_e, 2),
    )
    for stage, r in plan:
        stage(r)

    c_in = []
    for r in (1, 2, 3):
        c_in.append(go(remote(csum, csr.at[r], c_s.at[r], c_r.at[r], dev(dx=r))))
    for cp in c_in:
        cp.wait_recv()
    sums = csum[...] + csr[1] + csr[2] + csr[3]
    h_out = []
    for gi in (0, 1):
        hs[gi] = sums[:, gi * SLOTS : (gi + 1) * SLOTS]
    for gi in (0, 1):
        for cd in (0, 1):
            cp = remote(
                hs.at[gi], hsr.at[y], h_s.at[gi, cd], h_r.at[y],
                (z * 4 + 2 * c + gi, 2 * x + cd),
            )
            mine = jnp.logical_and(y == 2 * c + gi, c == cd)
            h_out.append((cp, mine))

            @pl.when(jnp.logical_not(mine))
            def _():
                cp.start()

            @pl.when(mine)
            def _():
                hsr[y] = hs[gi]

    for r in ORDER:
        f_in[r].wait_recv()
    out_ref[...] = (
        res[...].astype(F32) + fown[...] + frecv[1].astype(F32) + frecv[2].astype(F32)
        + frecv[3].astype(F32)
    ).astype(BF)

    for src in range(4):
        @pl.when(jnp.logical_not(jnp.logical_and(src == y, y // 2 == c)))
        def _():
            remote(hs.at[0], hsr.at[src], h_s.at[0, 0], h_r.at[src], peer).wait_recv()

    hm_ref[...] = (hsr[0] + hsr[1] + hsr[2] + hsr[3])[0:1, :] / TOKENS

    for cp in sent:
        cp.wait_send()
    for cp, mine in h_out:
        @pl.when(jnp.logical_not(mine))
        def _():
            cp.wait_send()

    @pl.when(ct != c)
    def _():
        wi_peer.wait_send()

    def drain(h, _):
        for i in (1, 2):
            for cp in back(i, h):
                cp.wait_send()
        swap(h).wait_send()
        return 0

    lax.fori_loop(0, HEADS, drain, 0)


def local(resid, queries, keys, values, doc_ids, out_proj, ffn_gain, w_in, w_out, hot_index,
          hot_blocks):
    dma = pltpu.SemaphoreType.DMA
    V = pltpu.VMEM
    hbm = pl.BlockSpec(memory_space=pl.ANY)
    vm = pl.BlockSpec(memory_space=pltpu.VMEM)
    sm = pl.BlockSpec(memory_space=pltpu.SMEM)
    scratch = [
        V((3, HEADS, TOK, 128), BF), V((4, HEADS, TOK, 128), BF), V((4, HEADS, TOK, 128), BF),
        V((4, 8, TOK), F32), V((3, 8, TOK), F32), V((4, TOK, 128), F32),
        V((128, TOK), F32), V((HEADS, 128, TOK), F32), V((HEADS, 8, TOK), F32),
        V((2, HEADS, 128, TOK), BF), V((2, HEADS, 8, TOK), F32),
        V((2, HEADS, 128, TOK), BF), V((2, HEADS, 8, TOK), F32),
        V((2, HEADS, TOK, 128), BF), V((4, 2 * WID, WID), BF), V((TOK, WID), BF),
        V((4, TOK, WID), BF), V((4, TOK, WID), BF),
        V((WID, NEUR), BF), V((NEUR, WID), BF), V((WID, SLOTS), BF),
        V((2 * WID, 2 * SLOTS), BF), V((4 * SLOTS, WID), BF),
        V((8, 8, TOK), F32), V((4, 2, TOK, WID), BF), V((4, TOK, 2 * SLOTS), F32),
        V((4, TOK, 2 * SLOTS), BF), V((4, 4, 64, 2 * SLOTS), BF), V((4, 2, TOK, 2 * SLOTS), BF),
        V((TOK, WID), F32), V((4, TOK, WID), BF), V((4, TOK, WID), BF),
        V((8, 2 * SLOTS), F32), V((4, 8, 2 * SLOTS), F32), V((2, 8, SLOTS), F32),
        V((4, 8, SLOTS), F32),
        dma((2, 4, HEADS)), dma((2, 4, HEADS)), dma((3, HEADS)), dma((3, HEADS)),
        dma((6,)), dma((6,)), dma((2, 2, HEADS)), dma((2, 2, HEADS)),
        dma((HEADS,)), dma((HEADS,)), dma((4,)), dma((4,)), dma((4,)), dma((4,)), dma((4,)),
        dma((3,)), dma((3, HEADS)), dma((4,)), dma((2, 2)), dma((4,)), dma((4,)),
        dma((8,)), dma((8,)), dma((4,)), dma((4,)), dma((4,)), dma((4,)),
        dma((4, 4)), dma((4, 4)), dma((4, 4)), dma((4, 4)), dma((4,)), dma((4,)),
        dma((4,)), dma((4,)), dma((4,)), dma((4,)), dma((2, 2)), dma((4,)),
    ]
    return pl.pallas_call(
        kernel,
        out_shape=(
            jax.ShapeDtypeStruct((TOK, WID), BF), jax.ShapeDtypeStruct((1, SLOTS), F32),
        ),
        in_specs=[hbm, hbm, hbm, hbm, vm, hbm, vm, hbm, hbm, vm, sm],
        out_specs=(vm, vm),
        scratch_shapes=scratch,
        compiler_params=pltpu.CompilerParams(
            collective_id=0, has_side_effects=True, vmem_limit_bytes=60 * 2**20
        ),
        name="layer",
    )(
        queries, keys, values, resid, doc_ids.reshape(1, TOK), out_proj,
        ffn_gain.reshape(1, WID), w_in, w_out, hot_index, hot_blocks,
    )


def solution(mesh):
    return jax.shard_map(
        local,
        mesh=mesh,
        in_specs=(
            P("seq", "mp"), P("seq", "mp"), P("seq", "mp"), P("seq", "mp"), P("seq"),
            P("mp", None), P("mp"), P("mp", "seq"), P("seq", "mp"), P("seq", None), P("seq"),
        ),
        out_specs=(P("seq", "mp"), P("seq", None)),
        check_vma=False,
    )
```

```python
import jax
import jax.numpy as jnp
from jax import lax
from jax.experimental import pallas as pl
from jax.experimental.pallas import tpu as pltpu
from jax.sharding import PartitionSpec as P

HEAD_DIM = 128
HEADS = 5
TOK = 256
WID = 640
SLOTS = 384
BLOCK = 128
NEUR = 864
D = 5120
TOKENS = 4096
EPS = 1e-05
LOW = -1e9
MASKED = -2e9
SCALE2 = HEAD_DIM ** (-0.5) * 1.4426950408889634
BF = jnp.bfloat16
F32 = jnp.float32
ORDER = (1, 3, 2)


def dot(a, b, dims):
    return lax.dot_general(a, b, (dims, ((), ())), preferred_element_type=F32)


def kernel(
    q_ref, k_ref, v_ref, resid_ref, doc_ref, oproj_ref, gain_ref, win_ref, wout_ref, hidx_ref,
    hblk_ref, out_ref, hm_ref,
    qb, kb, vb, drow, qrow, kcol, accw, acc0, st0, osend, ssend, orecv, srecv, att, wo, res,
    psend, precv, wi_own, wo_own, hin, win, wou, sqs, inv_row, inv_col, nb, prebuf, presend,
    prerecv, ab, fown, fsend, frecv, csum, csr, hs, hsr,
    kv_s, kv_r, q_s, q_r, d_s, d_r, o_s, o_r, a_s, a_r, wo_s, wo_r, wo_l, p_s, p_r, l_s, own_l,
    wi_s, wi_r, wu_s, wu_r, sq_s, sq_r, iv_s, iv_r, n_s, n_r, nd_s, nd_r, rs_s, rs_r, ag_s, ag_r,
    ad_s, ad_r, f_s, f_r, c_s, c_r, h_s, h_r,
):
    s = lax.axis_index("seq")
    m = lax.axis_index("mp")
    z, y, x, c = s // 4, s % 4, m // 2, m % 2

    def dev(dz=0, dy=0, dx=0, dc=0):
        return (((z + dz) % 4) * 4 + (y + dy) % 4, ((x + dx) % 4) * 2 + (c + dc) % 2)

    def remote(src, dst, ss, rs, device):
        return pltpu.make_async_remote_copy(
            src_ref=src, dst_ref=dst, send_sem=ss, recv_sem=rs, device_id=device,
            device_id_type=pl.DeviceIdType.MESH,
        )

    peer = dev(dc=1)
    sent = []

    def go(cp):
        cp.start()
        sent.append(cp)
        return cp

    def lane(ref, h):
        return ref.at[:, h * HEAD_DIM : (h + 1) * HEAD_DIM]

    loads = []
    for h in range(HEADS):
        for j, (src, dst) in enumerate(((q_ref, qb), (k_ref, kb), (v_ref, vb))):
            cp = pltpu.make_async_copy(lane(src, h), dst.at[0, h], own_l.at[j, h])
            cp.start()
            loads.append(cp)
    big = [
        pltpu.make_async_copy(win_ref, wi_own, l_s.at[0]),
        pltpu.make_async_copy(wout_ref, wo_own, l_s.at[1]),
        pltpu.make_async_copy(resid_ref, res, l_s.at[2]),
    ]
    for cp in big:
        cp.start()

    barrier = pltpu.get_barrier_semaphore()
    friends = [peer]
    for r in (1, 2, 3):
        friends += [dev(dy=r), dev(dy=r, dc=1), dev(dz=r), dev(dx=r), dev(dx=r, dc=1)]
    for f in friends:
        pl.semaphore_signal(barrier, inc=1, device_id=f, device_id_type=pl.DeviceIdType.MESH)
    doc_here = jnp.broadcast_to(doc_ref[...].astype(F32), (8, TOK))
    drow[0] = doc_here
    qrow[0] = doc_here
    pl.semaphore_wait(barrier, len(friends))
    for cp in loads:
        cp.wait()

    doc_in = []
    for r in (1, 2, 3):
        doc_in.append(go(remote(drow.at[0], drow.at[r], d_s.at[r], d_r.at[r], dev(dy=r))))
    for r in (1, 2):
        doc_in.append(go(remote(drow.at[0], qrow.at[r], d_s.at[3 + r], d_r.at[3 + r], dev(dz=-r))))

    def direct(h):
        return [
            remote(buf.at[0, h], buf.at[r, h], kv_s.at[j, r, h], kv_r.at[j, r, h], dev(dy=r))
            for r in (1, 3) for j, buf in enumerate((kb, vb))
        ]

    def relay(h):
        return [
            remote(kb.at[1, h], kb.at[2, h], kv_s.at[0, 2, h], kv_r.at[0, 2, h], dev(dy=1)),
            remote(vb.at[3, h], vb.at[2, h], kv_s.at[1, 2, h], kv_r.at[1, 2, h], dev(dy=3)),
        ]

    def ask(h):
        return [
            remote(qb.at[0, h], qb.at[r, h], q_s.at[r, h], q_r.at[r, h], dev(dz=-r)) for r in (1, 2)
        ]

    for h in (0, 1):
        for cp in direct(h):
            cp.start()
    for h in range(HEADS):
        for cp in ask(h):
            cp.start()

    wo_loc, wo_rem = [], []
    rows_c = pl.ds(pl.multiple_of(c * WID, 128), WID)
    for d in range(4):
        mine = pl.ds(pl.multiple_of((2 * d + c) * WID, 128), WID)
        theirs = pl.ds(pl.multiple_of((2 * d + 1 - c) * WID, 128), WID)
        cp = pltpu.make_async_copy(oproj_ref.at[:, mine], wo.at[d, rows_c, :], wo_l.at[d])
        cp.start()
        wo_loc.append(cp)
        wo_rem.append(
            go(remote(oproj_ref.at[:, theirs], wo.at[d, rows_c, :], wo_s.at[d], wo_r.at[d], peer))
        )

    for cp in big:
        cp.wait()
    live = lax.broadcasted_iota(jnp.int32, (1, SLOTS), 1) < BLOCK * hblk_ref[0]
    want = jnp.where(live, hidx_ref[...], -1)
    pick = (lax.broadcasted_iota(jnp.int32, (NEUR, SLOTS), 0) == want).astype(F32).astype(BF)
    hin[...] = dot(wi_own[...], pick, ((0,), (0,))).astype(BF)
    my_rows = pl.ds(pl.multiple_of(y * SLOTS, 128), SLOTS)
    wou[my_rows, :] = dot(pick, wo_own[...], ((0,), (0,))).astype(BF)
    ct = y // 2
    left, right = (y + 3) % 4, (y + 1) % 4

    def hot_cols(g):
        return pl.ds(pl.multiple_of((g % 2) * SLOTS, 128), SLOTS)

    win_dst = win.at[rows_c, hot_cols(y)]

    @pl.when(ct == c)
    def _():
        win[rows_c, hot_cols(y)] = hin[...]

    wi_peer = remote(hin, win_dst, wi_s.at[0], wi_r.at[y % 2, c], peer)

    @pl.when(ct != c)
    def _():
        wi_peer.start()

    wi_out = [
        remote(hin, win_dst, wi_s.at[r], wi_r.at[y % 2, c], (z * 4 + (y + r) % 4, 2 * x + ct))
        for r in (1, 3)
    ]
    wu_out = [
        remote(wou.at[my_rows], wou.at[my_rows], wu_s.at[r], wu_r.at[r], dev(dy=r)) for r in (1, 3)
    ]

    def pass_in(j):
        g = (left, right)[j]
        part = win.at[j * WID : (j + 1) * WID, hot_cols(g)]
        return g // 2 == c, remote(
            part, part, wi_s.at[4 + j], wi_r.at[g % 2, j], dev(dy=(1, 3)[j])
        )

    def pass_out(j):
        g = (left, right)[j]
        part = wou.at[pl.ds(pl.multiple_of(g * SLOTS + j * (SLOTS // 2), 64), SLOTS // 2)]
        return remote(part, part, wu_s.at[2 * j], wu_r.at[2 * j], dev(dy=(1, 3)[j]))

    for cp in doc_in:
        cp.wait_recv()
    for r in range(4):
        kcol[r] = jnp.transpose(jnp.broadcast_to(drow[r][0:1, :], (128, TOK)))

    def step(h, i, r, qd, top, total, causal):
        sc = dot(kb[r, h], qb[i, h], ((1,), (1,)))
        kd = kcol[r]
        mask = jnp.concatenate([kd, kd], axis=1) == qd
        if causal:
            key_at = lax.broadcasted_iota(jnp.int32, (TOK, TOK), 0)
            query_at = lax.broadcasted_iota(jnp.int32, (TOK, TOK), 1)
            mask = mask & (key_at <= query_at)
        sc = jnp.where(mask, sc, MASKED)
        new = jnp.maximum(top, jnp.max(sc, axis=0, keepdims=True))
        p = jnp.exp2((sc - new) * SCALE2)
        fade = jnp.exp2((top - new) * SCALE2)
        total = total * fade + jnp.sum(p, axis=0, keepdims=True)
        accw[...] = accw[...] * fade + dot(vb[r, h], p.astype(BF), ((0,), (0,)))
        return new, total

    low = jnp.full((1, TOK), LOW, F32)
    zero = jnp.zeros((1, TOK), F32)

    def both(top, total):
        row = lax.broadcasted_iota(jnp.int32, (8, TOK), 0)
        return jnp.where(row == 0, top, total)

    def back(i, h):
        return (
            remote(
                osend.at[i - 1, h], orecv.at[i - 1, h], o_s.at[0, i - 1, h], o_r.at[0, i - 1, h],
                (((z + i) % 4) * 4 + y, m),
            ),
            remote(
                ssend.at[i - 1, h], srecv.at[i - 1, h], o_s.at[1, i - 1, h], o_r.at[1, i - 1, h],
                (((z + i) % 4) * 4 + y, m),
            ),
        )

    def head(h, _):
        @pl.when(h + 2 < HEADS)
        def _():
            for cp in direct(h + 2):
                cp.start()

        @pl.when(h + 1 < HEADS)
        def _():
            pass_on(h + 1)

        @pl.when(h == HEADS - 2)
        def _():
            for cp in wi_out + wu_out:
                cp.start()

        for cp in ask(h):
            cp.wait_recv()
        for cp in relay(h):
            cp.wait_recv()

        def away(t, _):
            i = 2 - t
            qd = jnp.where(z + i <= 3, qrow[i][0:1, :], -5.0)
            accw[...] = jnp.zeros_like(accw)

            def visit(n, carry):
                r = jnp.where(jnp.logical_and(i == 2, n > 0), y + n, n)
                return step(h, i, r, qd, *carry, False)

            top, total = lax.fori_loop(0, jnp.where(i == 2, 4 - y, 4), visit, (low, zero))
            osend[i - 1, h] = accw[...].astype(BF)
            ssend[i - 1, h] = both(top, total)
            for cp in back(i, h):
                cp.start()
            return 0

        lax.fori_loop(0, 2, away, 0)
        accw[...] = jnp.zeros_like(accw)
        qd = qrow[0][0:1, :]
        carry = step(h, 0, 0, qd, low, zero, True)
        top, total = lax.fori_loop(
            1, y + 1, lambda r, carry: step(h, 0, r, qd, *carry, False), carry
        )
        acc0[h] = accw[...]
        st0[h] = both(top, total)
        return 0

    def pass_on(h):
        for cp in direct(h):
            cp.wait_recv()
        for cp in relay(h):
            cp.start()

    pass_on(0)
    lax.fori_loop(0, HEADS, head, 0)

    def swap(h):
        return remote(att.at[c, h], att.at[c, h], a_s.at[h], a_r.at[h], peer)

    def merge(h, _):
        for i in (1, 2):
            for cp in back(i, h):
                cp.wait_recv()
        t0, t1, t2 = st0[h][0:1, :], srecv[0, h][0:1, :], srecv[1, h][0:1, :]
        n0, n1, n2 = st0[h][1:2, :], srecv[0, h][1:2, :], srecv[1, h][1:2, :]
        top = jnp.maximum(t0, jnp.maximum(t1, t2))
        f0 = jnp.exp2((t0 - top) * SCALE2)
        f1 = jnp.exp2((t1 - top) * SCALE2)
        f2 = jnp.exp2((t2 - top) * SCALE2)
        inv = 1.0 / (n0 * f0 + n1 * f1 + n2 * f2)
        mixed = (
            acc0[h] * (f0 * inv)
            + orecv[0, h].astype(F32) * (f1 * inv)
            + orecv[1, h].astype(F32) * (f2 * inv)
        )
        att[c, h] = jnp.transpose(mixed).astype(BF)
        swap(h).start()
        return 0

    lax.fori_loop(0, HEADS, merge, 0)

    for cp in wo_loc:
        cp.wait()
    for cp in wo_rem:
        cp.wait_recv()
    for h in range(HEADS):
        remote(att.at[1 - c, h], att.at[1 - c, h], a_s.at[h], a_r.at[h], peer).wait_recv()
    both_att = jnp.concatenate([att[i, h] for i in (0, 1) for h in range(HEADS)], axis=1)
    p_in = []
    for r in (2, 1, 3):
        psend[r] = dot(both_att, wo[(x + r) % 4], ((1,), (0,))).astype(BF)
        p_in.append(go(remote(psend.at[r], precv.at[r], p_s.at[r], p_r.at[r], dev(dx=r))))
    fown[...] = dot(both_att, wo[x], ((1,), (0,))) + res[...].astype(F32)

    for j in (0, 1):
        here, cp = pass_in(j)

        @pl.when(here)
        def _():
            cp.wait_recv()
            cp.start()

    for cp in p_in:
        cp.wait_recv()
    state = (
        fown[...] + precv[1].astype(F32) + precv[2].astype(F32) + precv[3].astype(F32)
    ).astype(BF)
    res[...] = state

    wide = state.astype(F32)
    gain = gain_ref[...].astype(F32).reshape(1, WID)
    nb[0, c] = (wide * gain).astype(BF)
    square = wide * wide
    high = square.astype(BF)
    rest = (square - high.astype(F32)).astype(BF)
    ones = jnp.ones((8, WID), BF)
    sqs[0] = dot(ones, high, ((1,), (1,))) + dot(ones, rest, ((1,), (1,)))
    n_in, nd_in, iv_in, sq_in = {}, {}, {}, []
    nd_in[0] = go(remote(nb.at[0, c], nb.at[0, c], nd_s.at[0], nd_r.at[0], peer))
    for r in ORDER:
        n_in[r] = go(remote(nb.at[0, c], nb.at[r, c], n_s.at[r], n_r.at[r], dev(dz=r)))
    for j in range(1, 8):
        cp = remote(
            sqs.at[0], sqs.at[j], sq_s.at[j], sq_r.at[j], dev(dx=j // 2, dc=j % 2)
        )
        sq_in.append(go(cp))

    for cp in wu_out:
        cp.wait_recv()
    for j in (0, 1):
        go(pass_out(j))

    for gi in (0, 1):
        for cs in (0, 1):
            g = 2 * c + gi
            had = jnp.logical_or(
                jnp.logical_and(g == y, c == cs), g == (left, right)[cs]
            )

            @pl.when(jnp.logical_not(had))
            def _():
                remote(hin, win_dst, wi_s.at[0], wi_r.at[gi, cs], peer).wait_recv()

    csum[...] = jnp.zeros_like(csum)
    rs_in, ag_in, ad_in, f_in = {}, {}, {}, {}
    parts = ((0, 0, 128), (1, 0, TOK), (3, 0, TOK), (2, 0, TOK), (0, 128, 128))

    def quarter(b, at):
        _, first, n = parts[b]
        return pl.ds(pl.multiple_of(first + at * (n // 4), 32), n // 4)

    def columns_of(r, row):
        inv_col[r] = jnp.transpose(jnp.broadcast_to(row, (128, TOK)))

    def stage_n(b):
        for cp in sq_in:
            cp.wait_recv()
        squares = sqs[0]
        for j in range(1, 8):
            squares = squares + sqs[j]
        inv_row[0] = lax.rsqrt(squares / D + EPS)
        for r in ORDER:
            iv_in[r] = go(
                remote(inv_row.at[0], inv_row.at[r], iv_s.at[r], iv_r.at[r], dev(dz=r))
            )
        columns_of(0, inv_row[0][0:1, :])

    def stage_a(b):
        r = parts[b][0]
        n_in[r].wait_recv()
        nd_in[r] = go(remote(nb.at[r, c], nb.at[r, c], nd_s.at[r], nd_r.at[r], peer))

    def stage_b(b):
        r, first, n = parts[b]
        if b < 4:
            nd_in[r].wait_recv()
        at = slice(first, first + n)
        rows = jnp.concatenate([nb[r, 0, at], nb[r, 1, at]], axis=1)
        pre = dot(rows, win[...], ((1,), (0,)))
        prebuf[r, at] = pre
        presend[r, at] = pre.astype(BF)
        for e in (2, 1, 3):
            rs_in[b, e] = go(
                remote(
                    presend.at[r, quarter(b, (x + e) % 4)], prerecv.at[b, e, 0 : n // 4],
                    rs_s.at[b, e], rs_r.at[b, e], dev(dx=e),
                )
            )

    def stage_c(b):
        r, first, n = parts[b]
        for e in (1, 3, 2):
            rs_in[b, e].wait_recv()
        if r:
            iv_in[r].wait_recv()
            columns_of(r, inv_row[r][0:1, :])
        here = quarter(b, x)
        q = slice(0, n // 4)
        pre = (
            prebuf[r, here, :] + prerecv[b, 1, q].astype(F32) + prerecv[b, 2, q].astype(F32)
            + prerecv[b, 3, q].astype(F32)
        )
        factor = inv_col[r, here, :]
        active = jnp.maximum(pre, 0.0) * jnp.concatenate([factor] * 6, axis=1)
        csum[...] += jnp.sum(active, axis=0, keepdims=True)
        ab[r, c, here, :] = active.astype(BF)
        for e in (2, 1, 3):
            ag_in[b, e] = go(
                remote(
                    ab.at[r, c, here], ab.at[r, c, here], ag_s.at[b, e], ag_r.at[b, e], dev(dx=e)
                )
            )

    def stage_d(b):
        r, first, n = parts[b]
        for e in (1, 3, 2):
            ag_in[b, e].wait_recv()
        block = ab.at[r, c, first : first + n]
        ad_in[b] = go(remote(block, block, ad_s.at[b], ad_r.at[b], peer))

    def stage_e(b):
        r, first, n = parts[b]
        if b == 0:
            wu_relayed = (pass_out(0), pass_out(1))
            for cp in wu_relayed:
                cp.wait_recv()
        ad_in[b].wait_recv()
        at = slice(first, first + n)
        rows = jnp.concatenate([ab[r, 0, at], ab[r, 1, at]], axis=1)
        part = dot(rows, wou[...], ((1,), (0,)))
        if r == 0:
            fown[at] = part + res[at].astype(F32)
        else:
            fsend[r] = part.astype(BF)
            f_in[r] = go(remote(fsend.at[r], frecv.at[r], f_s.at[r], f_r.at[r], dev(dz=-r)))

    stage = {"n": stage_n, "a": stage_a, "b": stage_b, "c": stage_c, "d": stage_d, "e": stage_e}
    plan = "b0 n0 c0 a1 b1 d0 a2 b2 c1 e0 a3 b3 c2 d1 b4 c3 d2 e1 c4 d3 e2 d4 e3"
    for word in plan.split():
        stage[word[0]](int(word[1]))

    c_in = []
    for r in (1, 2, 3):
        c_in.append(go(remote(csum, csr.at[r], c_s.at[r], c_r.at[r], dev(dx=r))))
    for cp in c_in:
        cp.wait_recv()
    sums = csum[...] + csr[1] + csr[2] + csr[3]
    h_out = []
    for gi in (0, 1):
        hs[gi] = sums[:, gi * SLOTS : (gi + 1) * SLOTS]
    for gi in (0, 1):
        for cd in (0, 1):
            cp = remote(
                hs.at[gi], hsr.at[y], h_s.at[gi, cd], h_r.at[y],
                (z * 4 + 2 * c + gi, 2 * x + cd),
            )
            mine = jnp.logical_and(y == 2 * c + gi, c == cd)
            h_out.append((cp, mine))

            @pl.when(jnp.logical_not(mine))
            def _():
                cp.start()

            @pl.when(mine)
            def _():
                hsr[y] = hs[gi]

    stage_e(4)
    for r in ORDER:
        f_in[r].wait_recv()
    out_ref[...] = (
        fown[...] + frecv[1].astype(F32) + frecv[2].astype(F32) + frecv[3].astype(F32)
    ).astype(BF)

    for src in range(4):
        @pl.when(jnp.logical_not(jnp.logical_and(src == y, y // 2 == c)))
        def _():
            remote(hs.at[0], hsr.at[src], h_s.at[0, 0], h_r.at[src], peer).wait_recv()

    hm_ref[...] = (hsr[0] + hsr[1] + hsr[2] + hsr[3])[0:1, :] / TOKENS

    for cp in sent:
        cp.wait_send()
    for cp, mine in h_out:
        @pl.when(jnp.logical_not(mine))
        def _():
            cp.wait_send()

    @pl.when(ct != c)
    def _():
        wi_peer.wait_send()

    for cp in wi_out + wu_out:
        cp.wait_send()
    for j in (0, 1):
        here, cp = pass_in(j)

        @pl.when(here)
        def _():
            cp.wait_send()

    def drain(h, _):
        for cp in direct(h) + relay(h) + ask(h):
            cp.wait_send()
        for i in (1, 2):
            for cp in back(i, h):
                cp.wait_send()
        swap(h).wait_send()
        return 0

    lax.fori_loop(0, HEADS, drain, 0)


def local(resid, queries, keys, values, doc_ids, out_proj, ffn_gain, w_in, w_out, hot_index,
          hot_blocks):
    dma = pltpu.SemaphoreType.DMA
    V = pltpu.VMEM
    hbm = pl.BlockSpec(memory_space=pl.ANY)
    vm = pl.BlockSpec(memory_space=pltpu.VMEM)
    sm = pl.BlockSpec(memory_space=pltpu.SMEM)
    scratch = [
        V((3, HEADS, TOK, 128), BF), V((4, HEADS, TOK, 128), BF), V((4, HEADS, TOK, 128), BF),
        V((4, 8, TOK), F32), V((3, 8, TOK), F32), V((4, TOK, 128), F32),
        V((128, TOK), F32), V((HEADS, 128, TOK), F32), V((HEADS, 8, TOK), F32),
        V((2, HEADS, 128, TOK), BF), V((2, HEADS, 8, TOK), F32),
        V((2, HEADS, 128, TOK), BF), V((2, HEADS, 8, TOK), F32),
        V((2, HEADS, TOK, 128), BF), V((4, 2 * WID, WID), BF), V((TOK, WID), BF),
        V((4, TOK, WID), BF), V((4, TOK, WID), BF),
        V((NEUR, WID), BF), V((NEUR, WID), BF), V((WID, SLOTS), BF),
        V((2 * WID, 2 * SLOTS), BF), V((4 * SLOTS, WID), BF),
        V((8, 8, TOK), F32), V((4, 8, TOK), F32), V((4, TOK, 128), F32), V((4, 2, TOK, WID), BF),
        V((4, TOK, 2 * SLOTS), F32),
        V((4, TOK, 2 * SLOTS), BF), V((5, 4, 64, 2 * SLOTS), BF), V((4, 2, TOK, 2 * SLOTS), BF),
        V((TOK, WID), F32), V((4, TOK, WID), BF), V((4, TOK, WID), BF),
        V((8, 2 * SLOTS), F32), V((4, 8, 2 * SLOTS), F32), V((2, 8, SLOTS), F32),
        V((4, 8, SLOTS), F32),
        dma((2, 4, HEADS)), dma((2, 4, HEADS)), dma((3, HEADS)), dma((3, HEADS)),
        dma((6,)), dma((6,)), dma((2, 2, HEADS)), dma((2, 2, HEADS)),
        dma((HEADS,)), dma((HEADS,)), dma((4,)), dma((4,)), dma((4,)), dma((4,)), dma((4,)),
        dma((3,)), dma((3, HEADS)), dma((6,)), dma((2, 2)), dma((4,)), dma((4,)),
        dma((8,)), dma((8,)), dma((4,)), dma((4,)), dma((4,)), dma((4,)), dma((4,)), dma((4,)),
        dma((5, 4)), dma((5, 4)), dma((5, 4)), dma((5, 4)), dma((5,)), dma((5,)),
        dma((4,)), dma((4,)), dma((4,)), dma((4,)), dma((2, 2)), dma((4,)),
    ]
    return pl.pallas_call(
        kernel,
        out_shape=(
            jax.ShapeDtypeStruct((TOK, WID), BF), jax.ShapeDtypeStruct((1, SLOTS), F32),
        ),
        in_specs=[hbm, hbm, hbm, hbm, vm, hbm, vm, hbm, hbm, vm, sm],
        out_specs=(vm, vm),
        scratch_shapes=scratch,
        compiler_params=pltpu.CompilerParams(
            collective_id=0, has_side_effects=True, vmem_limit_bytes=60 * 2**20
        ),
        name="layer",
    )(
        queries, keys, values, resid, doc_ids.reshape(1, TOK), out_proj,
        ffn_gain, w_in.T, w_out, hot_index, hot_blocks,
    )


def solution(mesh):
    return jax.shard_map(
        local,
        mesh=mesh,
        in_specs=(
            P("seq", "mp"), P("seq", "mp"), P("seq", "mp"), P("seq", "mp"), P("seq"),
            P("mp", None), P("mp"), P("mp", "seq"), P("seq", "mp"), P("seq", None), P("seq"),
        ),
        out_specs=(P("seq", "mp"), P("seq", None)),
        check_vma=False,
    )
```

```python
import jax
import jax.numpy as jnp
from jax import lax
from jax.experimental import pallas as pl
from jax.experimental.pallas import tpu as pltpu
from jax.sharding import PartitionSpec as P

HEAD_DIM = 128
HEADS = 5
TOK = 256
WID = 640
SLOTS = 384
BLOCK = 128
NEUR = 864
D = 5120
TOKENS = 4096
EPS = 1e-05
LOW = -1e9
MASKED = -2e9
SCALE2 = HEAD_DIM ** (-0.5) * 1.4426950408889634
BF = jnp.bfloat16
F32 = jnp.float32
ORDER = (1, 3, 2)
PLAN = (
    "t4", "b0", "s0", "t5", "t6", "r0", "t3", "a2", "b1", "a7", "n0", "c0", "b2", "b7", "r1",
    "a4", "d0", "b4", "r2", "r7", "a5", "c1", "g0", "w0", "b5", "a3", "a6", "c2", "c4", "c7",
    "b3", "d1", "r5", "b6", "d2", "g4", "d7", "r3", "e4", "g1", "c5", "r6", "e0", "e1", "g2",
    "g7", "c3", "e2", "d5", "c6", "h0", "e7", "d3", "g5", "d6", "e5", "g3", "g6", "e3", "e6",
)


def dot(a, b, dims):
    return lax.dot_general(a, b, (dims, ((), ())), preferred_element_type=F32)


def kernel(
    q_ref, k_ref, v_ref, resid_ref, doc_ref, oproj_ref, gain_ref, win_ref, wout_ref, hidx_ref,
    hblk_ref, out_ref, hm_ref,
    qb, kvb, drow, qrow, kcol, acc0, st0, osend, ssend, orecv, srecv, att, wo, res,
    psend, precv, prel, pnear, wi_own, wo_own, hin, win, wou, sqs, inv_row, inv_col, nb, prebuf,
    presend, prerecv, relrecv, relsend, ab, fown, fsend, frecv, csum, csr, hs, hsr,
    out_s, kv_r, q_r, o_r, p_r, l_s, own_l, wi_s, wi_r, n_r, nd_r, rel_r, rs_r, ag_r, fwd_r, ad_r,
    one_r, h_s, h_r,
):
    s = lax.axis_index("seq")
    m = lax.axis_index("mp")
    z, y, x, c = s // 4, s % 4, m // 2, m % 2

    def dev(dz=0, dy=0, dx=0, dc=0):
        return (((z + dz) % 4) * 4 + (y + dy) % 4, ((x + dx) % 4) * 2 + (c + dc) % 2)

    def remote(src, dst, ss, rs, device):
        return pltpu.make_async_remote_copy(
            src_ref=src, dst_ref=dst, send_sem=ss, recv_sem=rs, device_id=device,
            device_id_type=pl.DeviceIdType.MESH,
        )

    peer = dev(dc=1)

    def go(cp):
        cp.start()
        return cp

    def arrived(ref, sem):
        remote(ref, ref, sem, sem, peer).wait_recv()

    def gone(ref, sem):
        remote(ref, ref, sem, sem, peer).wait_send()

    (S_KV, S_Q, S_DK, S_DQ, S_O, S_A, S_WO, S_P, S_WU, S_SQ, S_IV, S_N, S_ND, S_X, S_AD, S_F,
     S_C) = [out_s.at[i] for i in range(17)]
    R_DK, R_DQ, R_A, R_WO, R_WU, R_WP, R_SQ, R_IV, R_F, R_C, R_WL = [
        one_r.at[i] for i in range(11)
    ]

    def lane(ref, h):
        return ref.at[:, h * HEAD_DIM : (h + 1) * HEAD_DIM]

    for h in range(HEADS):
        pltpu.make_async_copy(lane(k_ref, h), kvb.at[0, h, 0], own_l.at[0]).start()
        pltpu.make_async_copy(lane(v_ref, h), kvb.at[0, h, 1], own_l.at[0]).start()
        pltpu.make_async_copy(lane(q_ref, h), qb.at[0, h], own_l.at[1]).start()
    big = [
        pltpu.make_async_copy(win_ref, wi_own, l_s.at[0]),
        pltpu.make_async_copy(wout_ref, wo_own, l_s.at[1]),
        pltpu.make_async_copy(resid_ref, res, l_s.at[2]),
    ]
    for cp in big:
        cp.start()

    barrier = pltpu.get_barrier_semaphore()
    friends = [peer]
    for r in (1, 2, 3):
        friends += [dev(dy=r), dev(dy=r, dc=1), dev(dz=r), dev(dx=r), dev(dx=r, dc=1)]
    for f in friends:
        pl.semaphore_signal(barrier, inc=1, device_id=f, device_id_type=pl.DeviceIdType.MESH)
    doc_here = jnp.broadcast_to(doc_ref[...].astype(F32), (8, TOK))
    drow[0] = doc_here
    qrow[0] = doc_here
    pl.semaphore_wait(barrier, len(friends))
    for r in (1, 2, 3):
        go(remote(drow.at[0], drow.at[r], S_DK, R_DK, dev(dy=r)))
    for r in (1, 2):
        go(remote(drow.at[0], qrow.at[r], S_DQ, R_DQ, dev(dz=-r)))
    pltpu.make_async_copy(kvb.at[0], kvb.at[0], own_l.at[0]).wait()
    pltpu.make_async_copy(qb.at[0], qb.at[0], own_l.at[1]).wait()

    def direct(h):
        return [
            remote(kvb.at[0, h], kvb.at[r, h], S_KV, kv_r.at[r // 2, h], dev(dy=r)) for r in (1, 3)
        ]

    def relay(h):
        return [
            remote(kvb.at[1, h, 0], kvb.at[2, h, 0], S_KV, kv_r.at[2, h], dev(dy=1)),
            remote(kvb.at[3, h, 1], kvb.at[2, h, 1], S_KV, kv_r.at[2, h], dev(dy=3)),
        ]

    def ask(h):
        return [remote(qb.at[0, h], qb.at[r, h], S_Q, q_r.at[h], dev(dz=-r)) for r in (1, 2)]

    for h in range(HEADS):
        if h < 2:
            for cp in direct(h):
                cp.start()
        for cp in ask(h):
            cp.start()

    rows_c = pl.ds(pl.multiple_of(c * WID, 128), WID)

    def chunk(of):
        return oproj_ref.at[:, pl.ds(pl.multiple_of(of * WID, 128), WID)]

    rows_o = pl.ds(pl.multiple_of((1 - c) * WID, 128), WID)
    wo_loc = [
        pltpu.make_async_copy(chunk(2 * d + c), wo.at[d, rows_c, :], R_WL) for d in range(4)
    ]
    wo_rem = [
        remote(chunk(2 * d + 1 - c), wo.at[d, rows_c, :], S_WO, R_WO, peer) for d in range(4)
    ]

    ct = y // 2
    left, right = (y + 3) % 4, (y + 1) % 4

    def hot_cols(g):
        return pl.ds(pl.multiple_of((g % 2) * SLOTS, 128), SLOTS)

    win_dst = win.at[rows_c, hot_cols(y)]
    my_rows = pl.ds(pl.multiple_of(y * SLOTS, 128), SLOTS)
    wi_peer = remote(hin, win_dst, wi_s.at[0], wi_r.at[y % 2, c], peer)

    def choose():
        for cp in big:
            cp.wait()
        live = lax.broadcasted_iota(jnp.int32, (1, SLOTS), 1) < BLOCK * hblk_ref[0]
        want = jnp.where(live, hidx_ref[...], -1)
        pick = (lax.broadcasted_iota(jnp.int32, (NEUR, SLOTS), 0) == want).astype(F32).astype(BF)
        hin[...] = dot(wi_own[...], pick, ((0,), (0,))).astype(BF)
        wou[my_rows, :] = dot(pick, wo_own[...], ((0,), (0,))).astype(BF)

        @pl.when(ct == c)
        def _():
            win[rows_c, hot_cols(y)] = hin[...]

        @pl.when(ct != c)
        def _():
            wi_peer.start()

    wi_out = [
        remote(hin, win_dst, wi_s.at[r], wi_r.at[y % 2, c], (z * 4 + (y + r) % 4, 2 * x + ct))
        for r in (1, 3)
    ]
    wu_out = [
        remote(wou.at[my_rows], wou.at[my_rows], S_WU, R_WU, dev(dy=r)) for r in (1, 3)
    ]

    def pass_in(j):
        g = (left, right)[j]
        part = win.at[j * WID : (j + 1) * WID, hot_cols(g)]
        return g // 2 == c, remote(
            part, part, wi_s.at[4 + j], wi_r.at[g % 2, j], dev(dy=(1, 3)[j])
        )

    def pass_out(j):
        g = (left, right)[j]
        part = wou.at[pl.ds(pl.multiple_of(g * SLOTS + j * (SLOTS // 2), 64), SLOTS // 2)]
        return remote(part, part, S_WU, R_WP, dev(dy=(1, 3)[j]))

    choose()
    arrived(drow.at[1:4], R_DK)
    arrived(qrow.at[1:3], R_DQ)
    for r in range(4):
        kcol[r] = jnp.transpose(jnp.broadcast_to(drow[r][0:1, :], (128, TOK)))

    def pair(h, i, r, qd, causal=False):
        sc = dot(kvb[r, h, 0], qb[i, h], ((1,), (1,)))
        kd = kcol[r]
        mask = jnp.concatenate([kd, kd], axis=1) == qd
        if causal:
            key_at = lax.broadcasted_iota(jnp.int32, (TOK, TOK), 0)
            query_at = lax.broadcasted_iota(jnp.int32, (TOK, TOK), 1)
            mask = mask & (key_at <= query_at)
        sc = jnp.where(mask, sc, MASKED)
        top = jnp.maximum(jnp.max(sc, axis=0, keepdims=True), LOW)
        p = jnp.exp2((sc - top) * SCALE2)
        total = jnp.sum(p, axis=0, keepdims=True)
        return top, total, dot(kvb[r, h, 1], p.astype(BF), ((0,), (0,)))

    def together(results):
        top = results[0][0]
        for other, _, _ in results[1:]:
            top = jnp.maximum(top, other)
        total, acc = 0.0, 0.0
        for own, part, mixed in results:
            factor = jnp.exp2((own - top) * SCALE2)
            total = total + part * factor
            acc = acc + mixed * factor
        return top, total, acc

    def both(top, total):
        row = lax.broadcasted_iota(jnp.int32, (8, TOK), 0)
        return jnp.where(row == 0, top, total)

    def back(i, h):
        return (
            remote(
                osend.at[i - 1, h, 0:128], orecv.at[i - 1, h, 0:128], S_O, o_r.at[h],
                (((z + i) % 4) * 4 + y, m),
            ),
            remote(
                ssend.at[i - 1, h], srecv.at[i - 1, h], S_O, o_r.at[h],
                (((z + i) % 4) * 4 + y, m),
            ),
        )

    def head(h, _):
        @pl.when(h + 2 < HEADS)
        def _():
            for cp in direct(h + 2):
                cp.start()

        arrived(qb.at[1:3, h], q_r.at[h])
        q0 = qrow[0][0:1, :]
        q1 = jnp.where(z + 1 <= 3, qrow[1][0:1, :], -5.0)
        q2 = jnp.where(z + 2 <= 3, qrow[2][0:1, :], -5.0)

        def shared(n):
            if n == 0:
                return pair(h, 0, 0, q0, True)
            own = n <= y
            slot = jnp.where(own, n, jnp.where(n == y + 1, 0, n - 1))
            return pair(h, jnp.where(own, 0, 2), slot, jnp.where(own, q0, q2))

        near, mix = {}, {}
        for n in (0, 1, 3):
            near[n] = pair(h, 1, n, q1)
        for n in (0, 1, 4):
            mix[n] = shared(n)

        @pl.when(h + 1 < HEADS)
        def _():
            pass_on(h + 1)

        @pl.when(h == HEADS - 2)
        def _():
            for cp in wi_out:
                cp.start()

        arrived(kvb.at[2, h], kv_r.at[2, h])
        for n in (2, 3):
            mix[n] = shared(n)
        far = [
            (jnp.where(n <= y, LOW, mix[n][0]), mix[n][1], mix[n][2]) for n in (1, 2, 3)
        ] + [mix[4]]
        for i, parts_of in ((2, far), (1, None)):
            if i == 1:
                near[2] = pair(h, 1, 2, q1)
                parts_of = [near[n] for n in range(4)]
            top, total, acc = together(parts_of)
            osend[i - 1, h, 0:128] = acc.astype(BF)
            ssend[i - 1, h] = both(top, total)
            for cp in back(i, h):
                cp.start()
        top, total, acc = together(
            [mix[0]] + [(jnp.where(n <= y, mix[n][0], LOW), mix[n][1], mix[n][2]) for n in (1, 2, 3)]
        )
        acc0[h] = acc
        st0[h] = both(top, total)

        @pl.when(h == 0)
        def _():
            for cp in wo_loc + wo_rem:
                cp.start()

        return 0

    def pass_on(h):
        for cp in direct(h):
            cp.wait_recv()
        for cp in relay(h):
            cp.start()

    pass_on(0)
    lax.fori_loop(0, HEADS, head, 0)

    def swap(h):
        return remote(att.at[c, h], att.at[c, h], S_A, R_A, peer)

    def merge(h, _):
        arrived(orecv.at[:, h], o_r.at[h])
        t0, t1, t2 = st0[h][0:1, :], srecv[0, h][0:1, :], srecv[1, h][0:1, :]
        n0, n1, n2 = st0[h][1:2, :], srecv[0, h][1:2, :], srecv[1, h][1:2, :]
        top = jnp.maximum(t0, jnp.maximum(t1, t2))
        f0 = jnp.exp2((t0 - top) * SCALE2)
        f1 = jnp.exp2((t1 - top) * SCALE2)
        f2 = jnp.exp2((t2 - top) * SCALE2)
        inv = 1.0 / (n0 * f0 + n1 * f1 + n2 * f2)
        mixed = (
            acc0[h] * (f0 * inv)
            + orecv[0, h, 0:128].astype(F32) * (f1 * inv)
            + orecv[1, h, 0:128].astype(F32) * (f2 * inv)
        )
        att[c, h] = jnp.transpose(mixed).astype(BF)
        swap(h).start()
        return 0

    lax.fori_loop(0, HEADS, merge, 0)

    pltpu.make_async_copy(wo.at[:, rows_c, :], wo.at[:, rows_c, :], R_WL).wait()
    arrived(wo.at[:, rows_o, :], R_WO)
    arrived(att.at[1 - c], R_A)
    both_att = jnp.concatenate([att[i, h] for i in (0, 1) for h in range(HEADS)], axis=1)

    def span(k, j):
        return slice(128 * k + 64 * j, 128 * k + 64 * j + 64)

    def project(dx, k):
        return dot(both_att[128 * k : 128 * k + 128], wo[(x + dx) % 4], ((1,), (0,)))

    def across(k):
        psend[2, 128 * k : 128 * k + 128] = project(2, k).astype(BF)
        for j, e in ((0, 1), (1, 3)):
            go(remote(psend.at[2, span(k, j)], prel.at[k, j], S_P, p_r.at[k], dev(dx=e)))

    def beside(k):
        for j, e in ((0, 1), (1, 3)):
            pnear[j, 128 * k : 128 * k + 128] = project(e, k)
            rows = span(k, 1 - j)
            psend[e, rows] = pnear[j, rows].astype(BF)
            half = slice(64 - 64 * j, 128 - 64 * j)
            go(remote(psend.at[e, rows], precv.at[k, j, half], S_P, p_r.at[2 + k], dev(dx=e)))

    def onward(k):
        arrived(prel.at[k], p_r.at[k])
        for j, e in ((0, 1), (1, 3)):
            rows = span(k, j)
            psend[e, rows] = (pnear[j, rows] + prel[k, j].astype(F32)).astype(BF)
            half = slice(64 * j, 64 * j + 64)
            go(remote(psend.at[e, rows], precv.at[k, j, half], S_P, p_r.at[2 + k], dev(dx=e)))

    across(0)
    beside(0)
    across(1)

    for j in (0, 1):
        here, cp = pass_in(j)

        @pl.when(here)
        def _():
            cp.wait_recv()
            cp.start()

    for cp in wu_out:
        cp.start()

    onward(0)
    beside(1)
    for k in (0, 1):
        at = slice(128 * k, 128 * k + 128)
        fown[at] = project(0, k) + res[at].astype(F32)
    onward(1)

    n_in, nd_in = {}, {}

    def tokens(r, k):
        half = slice(128 * k, 128 * k + 128)
        n_in[r, k] = go(
            remote(nb.at[0, c, half], nb.at[r, c, half], S_N, n_r.at[r - 1, k], dev(dz=r))
        )

    def mate(r, k):
        half = nb.at[r, c, 128 * k : 128 * k + 128]
        nd_in[r, k] = go(remote(half, half, S_ND, nd_r.at[r, k], peer))

    gain = gain_ref[...].astype(F32).reshape(1, WID)

    def settle(k):
        at = slice(128 * k, 128 * k + 128)
        arrived(precv.at[k], p_r.at[2 + k])
        state = (fown[at] + precv[k, 0].astype(F32) + precv[k, 1].astype(F32)).astype(BF)
        res[at] = state
        nb[0, c, at] = (state.astype(F32) * gain).astype(BF)
        mate(0, k)

    settle(0)
    for r in (1, 3):
        tokens(r, 0)

    def stage_w(b):
        arrived(wou.at[0 : 2 * SLOTS], R_WU)
        for j in (0, 1):
            go(pass_out(j))

    for gi in (0, 1):
        for cs in (0, 1):
            g = 2 * c + gi
            had = jnp.logical_or(
                jnp.logical_and(g == y, c == cs), g == (left, right)[cs]
            )

            @pl.when(jnp.logical_not(had))
            def _():
                remote(hin, win_dst, wi_s.at[0], wi_r.at[gi, cs], peer).wait_recv()

    csum[...] = jnp.zeros_like(csum)
    parts = tuple(
        (r, 128 * k, 128)
        for r, k in ((0, 0), (0, 1), (1, 0), (3, 1), (2, 0), (2, 1), (1, 1), (3, 0))
    )

    plain = (4,)

    def quarter(b, at):
        _, first, n = parts[b]
        return pl.ds(pl.multiple_of(first + at * (n // 4), 32), n // 4)

    def eighth(b, at, j):
        _, first, n = parts[b]
        return pl.ds(pl.multiple_of(first + at * (n // 4) + j * (n // 8), 16), n // 8)

    def columns_of(r, row):
        inv_col[r] = jnp.transpose(jnp.broadcast_to(row, (128, TOK)))

    def stage_n(b):
        arrived(sqs.at[1:8], R_SQ)
        squares = sqs[0]
        for j in range(1, 8):
            squares = squares + sqs[j]
        inv_row[0] = lax.rsqrt(squares / D + EPS)
        for r in ORDER:
            go(remote(inv_row.at[0], inv_row.at[r], S_IV, R_IV, dev(dz=r)))
        columns_of(0, inv_row[0][0:1, :])

    def stage_a(b):
        r, first, _ = parts[b]
        if r:
            n_in[r, first // 128].wait_recv()
            mate(r, first // 128)

    def stage_b(b):
        r, first, n = parts[b]
        nd_in[r, first // 128].wait_recv()
        at = slice(first, first + n)
        rows = jnp.concatenate([nb[r, 0, at], nb[r, 1, at]], axis=1)
        pre = dot(rows, win[...], ((1,), (0,)))
        prebuf[r, at] = pre
        presend[r, at] = pre.astype(BF)
        h = n // 8
        if b in plain:
            for e in (2, 1, 3):
                go(
                    remote(
                        presend.at[r, quarter(b, (x + e) % 4)], prerecv.at[b, e - 1], S_X,
                        rs_r.at[b], dev(dx=e),
                    )
                )
            return
        for j, e in ((0, 1), (1, 3)):
            rest = slice(h - j * h, 2 * h - j * h)
            go(
                remote(
                    presend.at[r, eighth(b, (x + 2) % 4, j)], relrecv.at[b, j], S_X, rel_r.at[b],
                    dev(dx=e),
                )
            )
            go(
                remote(
                    presend.at[r, eighth(b, (x + e) % 4, 1 - j)], prerecv.at[b, j, rest], S_X,
                    rs_r.at[b], dev(dx=e),
                )
            )

    def stage_r(b):
        r, first, n = parts[b]
        h = n // 8
        arrived(relrecv.at[b], rel_r.at[b])
        for j, e in ((0, 1), (1, 3)):
            half = slice(j * h, j * h + h)
            there = eighth(b, (x + e) % 4, j)
            relsend[b, j] = (
                prebuf[r, there, :] + relrecv[b, j].astype(F32)
            ).astype(BF)
            go(remote(relsend.at[b, j], prerecv.at[b, j, half], S_X, rs_r.at[b], dev(dx=e)))

    def stage_c(b):
        r, first, n = parts[b]
        arrived(prerecv.at[b, 0 : 3 if b in plain else 2], rs_r.at[b])
        if b == 2:
            arrived(inv_row.at[1:4], R_IV)
        if r and first == 0:
            columns_of(r, inv_row[r][0:1, :])
        here = quarter(b, x)
        q = slice(0, n // 4)
        pre = (
            prebuf[r, here, :] + prerecv[b, 0, q].astype(F32) + prerecv[b, 1, q].astype(F32)
        )
        if b in plain:
            pre = pre + prerecv[b, 2].astype(F32)
        factor = inv_col[r, here, :]
        active = jnp.maximum(pre, 0.0) * jnp.concatenate([factor] * 6, axis=1)
        csum[...] += jnp.sum(active, axis=0, keepdims=True)
        ab[r, c, here, :] = active.astype(BF)
        for e in (2, 1, 3) if b in plain else (1, 3):
            go(remote(ab.at[r, c, here], ab.at[r, c, here], S_X, ag_r.at[b], dev(dx=e)))

    def stage_d(b):
        r, first, n = parts[b]
        arrived(ab.at[r, c, first : first + n // 2], ag_r.at[b])
        for j, e in ((0, 1), (1, 3)):
            block = ab.at[r, c, eighth(b, (x - e) % 4, j)]
            go(remote(block, block, S_X, fwd_r.at[b], dev(dx=e)))

    def stage_g(b):
        r, first, n = parts[b]
        if b in plain:
            arrived(ab.at[r, c, first : first + 3 * n // 4], ag_r.at[b])
        else:
            arrived(ab.at[r, c, first : first + n // 4], fwd_r.at[b])
        block = ab.at[r, c, first : first + n]
        go(remote(block, block, S_AD, ad_r.at[b], peer))

    def stage_e(b):
        r, first, n = parts[b]
        if b == 4:
            arrived(wou.at[0:SLOTS], R_WP)
        arrived(ab.at[r, 1 - c, first : first + n], ad_r.at[b])
        at = slice(first, first + n)
        rows = jnp.concatenate([ab[r, 0, at], ab[r, 1, at]], axis=1)
        part = dot(rows, wou[...], ((1,), (0,)))
        if r == 0:
            fown[at] = part + res[at].astype(F32)
        else:
            fsend[r, at] = part.astype(BF)
            go(remote(fsend.at[r, at], frecv.at[r, at], S_F, R_F, dev(dz=-r)))

    def stage_s(b):
        settle(1)
        wide = res[...].astype(F32)
        square = wide * wide
        high = square.astype(BF)
        rest = (square - high.astype(F32)).astype(BF)
        ones = jnp.ones((8, WID), BF)
        sqs[0] = dot(ones, high, ((1,), (1,))) + dot(ones, rest, ((1,), (1,)))
        for j in range(1, 8):
            go(remote(sqs.at[0], sqs.at[j], S_SQ, R_SQ, dev(dx=j // 2, dc=j % 2)))

    def stage_t(b):
        tokens(parts[b][0], parts[b][1] // 128)

    def stage_h(b):
        for r in (1, 2, 3):
            go(remote(csum, csr.at[r], S_C, R_C, dev(dx=r)))

    stage = {
        "n": stage_n, "a": stage_a, "b": stage_b, "r": stage_r, "c": stage_c, "d": stage_d,
        "g": stage_g, "e": stage_e, "h": stage_h, "s": stage_s, "t": stage_t, "w": stage_w,
    }
    for word in PLAN:
        stage[word[0]](int(word[1]))

    arrived(csr.at[1:4], R_C)
    sums = csum[...] + csr[1] + csr[2] + csr[3]
    h_out = []
    for gi in (0, 1):
        hs[gi] = sums[:, gi * SLOTS : (gi + 1) * SLOTS]
    for gi in (0, 1):
        for cd in (0, 1):
            cp = remote(
                hs.at[gi], hsr.at[y], h_s.at[gi, cd], h_r.at[y],
                (z * 4 + 2 * c + gi, 2 * x + cd),
            )
            mine = jnp.logical_and(y == 2 * c + gi, c == cd)
            h_out.append((cp, mine))

            @pl.when(jnp.logical_not(mine))
            def _():
                cp.start()

            @pl.when(mine)
            def _():
                hsr[y] = hs[gi]

    arrived(frecv.at[1:4], R_F)
    out_ref[...] = (
        fown[...] + frecv[1].astype(F32) + frecv[2].astype(F32) + frecv[3].astype(F32)
    ).astype(BF)

    for src in range(4):
        @pl.when(jnp.logical_not(jnp.logical_and(src == y, y // 2 == c)))
        def _():
            remote(hs.at[0], hsr.at[src], h_s.at[0, 0], h_r.at[src], peer).wait_recv()

    hm_ref[...] = (hsr[0] + hsr[1] + hsr[2] + hsr[3])[0:1, :] / TOKENS

    gone(kvb.at[0:3], S_KV)
    gone(qb.at[0:2], S_Q)
    gone(drow.at[0:3], S_DK)
    gone(drow.at[0:2], S_DQ)
    gone(orecv, S_O)
    gone(att.at[c], S_A)
    gone(wo.at[:, rows_c, :], S_WO)
    gone(psend.at[0:3], S_P)
    gone(wou.at[0 : 3 * SLOTS], S_WU)
    gone(sqs.at[1:8], S_SQ)
    gone(inv_row.at[1:4], S_IV)
    gone(fsend.at[1:4], S_N)
    gone(nb.at[0:2], S_ND)
    gone(ab.at[0:3], S_X)
    gone(presend, S_AD)
    gone(fsend.at[1:4], S_F)
    gone(csr.at[1:4], S_C)
    for cp, mine in h_out:
        @pl.when(jnp.logical_not(mine))
        def _():
            cp.wait_send()

    @pl.when(ct != c)
    def _():
        wi_peer.wait_send()

    for cp in wi_out:
        cp.wait_send()
    for j in (0, 1):
        here, cp = pass_in(j)

        @pl.when(here)
        def _():
            cp.wait_send()


def local(resid, queries, keys, values, doc_ids, out_proj, ffn_gain, w_in, w_out, hot_index,
          hot_blocks):
    dma = pltpu.SemaphoreType.DMA
    V = pltpu.VMEM
    hbm = pl.BlockSpec(memory_space=pl.ANY)
    vm = pl.BlockSpec(memory_space=pltpu.VMEM)
    sm = pl.BlockSpec(memory_space=pltpu.SMEM)
    scratch = [
        V((3, HEADS, TOK, 128), BF), V((4, HEADS, 2, TOK, 128), BF),
        V((4, 8, TOK), F32), V((3, 8, TOK), F32), V((4, TOK, 128), F32),
        V((HEADS, 128, TOK), F32), V((HEADS, 8, TOK), F32),
        V((2, HEADS, 144, TOK), BF), V((2, HEADS, 8, TOK), F32),
        V((2, HEADS, 144, TOK), BF), V((2, HEADS, 8, TOK), F32),
        V((2, HEADS, TOK, 128), BF), V((4, 2 * WID, WID), BF), V((TOK, WID), BF),
        V((4, TOK, WID), BF), V((2, 2, 128, WID), BF), V((2, 2, 64, WID), BF), V((2, TOK, WID), F32),
        V((NEUR, WID), BF), V((NEUR, WID), BF), V((WID, SLOTS), BF),
        V((2 * WID, 2 * SLOTS), BF), V((4 * SLOTS, WID), BF),
        V((8, 8, TOK), F32), V((4, 8, TOK), F32), V((4, TOK, 128), F32), V((4, 2, TOK, WID), BF),
        V((4, TOK, 2 * SLOTS), F32),
        V((4, TOK, 2 * SLOTS), BF), V((8, 3, 32, 2 * SLOTS), BF), V((8, 2, 16, 2 * SLOTS), BF),
        V((8, 2, 16, 2 * SLOTS), BF), V((4, 2, TOK, 2 * SLOTS), BF),
        V((TOK, WID), F32), V((4, TOK, WID), BF), V((4, TOK, WID), BF),
        V((8, 2 * SLOTS), F32), V((4, 8, 2 * SLOTS), F32), V((2, 8, SLOTS), F32),
        V((4, 8, SLOTS), F32),
        dma((17,)), dma((3, HEADS)), dma((HEADS,)), dma((HEADS,)), dma((4,)), dma((3,)), dma((2,)),
        dma((6,)), dma((2, 2)), dma((3, 2)), dma((4, 2)), dma((8,)), dma((8,)), dma((8,)),
        dma((8,)), dma((8,)), dma((11,)), dma((2, 2)), dma((4,)),
    ]
    return pl.pallas_call(
        kernel,
        out_shape=(
            jax.ShapeDtypeStruct((TOK, WID), BF), jax.ShapeDtypeStruct((1, SLOTS), F32),
        ),
        in_specs=[hbm, hbm, hbm, hbm, vm, hbm, vm, hbm, hbm, vm, sm],
        out_specs=(vm, vm),
        scratch_shapes=scratch,
        compiler_params=pltpu.CompilerParams(
            collective_id=0, has_side_effects=True, vmem_limit_bytes=60 * 2**20
        ),
        name="layer",
    )(
        queries, keys, values, resid, doc_ids.reshape(1, TOK), out_proj,
        ffn_gain, w_in.T, w_out, hot_index, hot_blocks,
    )


def solution(mesh):
    return jax.shard_map(
        local,
        mesh=mesh,
        in_specs=(
            P("seq", "mp"), P("seq", "mp"), P("seq", "mp"), P("seq", "mp"), P("seq"),
            P("mp", None), P("mp"), P("mp", "seq"), P("seq", "mp"), P("seq", None), P("seq"),
        ),
        out_specs=(P("seq", "mp"), P("seq", None)),
        check_vma=False,
    )
```

```python
import jax
import jax.numpy as jnp
from jax import lax
from jax.experimental import pallas as pl
from jax.experimental.pallas import tpu as pltpu
from jax.sharding import PartitionSpec as P

HEAD_DIM = 128
HEADS = 5
TOK = 256
WID = 640
SLOTS = 384
BLOCK = 128
NEUR = 864
D = 5120
TOKENS = 4096
EPS = 1e-05
LOW = -1e9
MASKED = -2e9
SCALE2 = HEAD_DIM ** (-0.5) * 1.4426950408889634
BF = jnp.bfloat16
F32 = jnp.float32
ORDER = (1, 3, 2)
PLAN = (
    "b0", "s0", "t7", "t6", "r0", "a2", "a3", "b1", "n0", "c0", "b2", "b3", "r1", "a7", "a6",
    "d0", "b7", "a4", "r2", "b6", "r3", "b4", "g0", "c1", "a5", "r7", "c2", "r6", "b5", "c3",
    "w0", "r4", "d1", "c7", "d2", "c6", "r5", "d3", "c4", "g1", "d7", "e0", "e1", "g2", "d6",
    "c5", "h0", "g3", "e2", "d4", "e3", "g6", "g7", "d5", "g4", "e6", "e7", "e4", "g5", "e5",
    "q2", "q3", "q6", "q7",
)


def dot(a, b, dims):
    return lax.dot_general(a, b, (dims, ((), ())), preferred_element_type=F32)


def kernel(
    q_ref, k_ref, v_ref, resid_ref, doc_ref, oproj_ref, gain_ref, win_ref, wout_ref, hidx_ref,
    hblk_ref, out_ref, hm_ref,
    qb, kvb, drow, qrow, kcol, acc0, st0, osend, ssend, orecv, srecv, att, wo, res,
    psend, precv, prel, pnear, wi_own, wo_own, hin, win, wou, sqs, inv_row, inv_col, nb, prebuf,
    presend, prerecv, relrecv, relsend, ab, fown, fsend, frecv, frel, fpart, csum, csr, hs, hsr,
    out_s, kv_r, q_r, o_r, p_r, l_s, own_l, wi_s, wi_r, n_r, nd_r, rel_r, rs_r, ag_r, fwd_r, ad_r,
    fr_r, one_r, h_s, h_r,
):
    s = lax.axis_index("seq")
    m = lax.axis_index("mp")
    z, y, x, c = s // 4, s % 4, m // 2, m % 2

    def dev(dz=0, dy=0, dx=0, dc=0):
        return (((z + dz) % 4) * 4 + (y + dy) % 4, ((x + dx) % 4) * 2 + (c + dc) % 2)

    def remote(src, dst, ss, rs, device):
        return pltpu.make_async_remote_copy(
            src_ref=src, dst_ref=dst, send_sem=ss, recv_sem=rs, device_id=device,
            device_id_type=pl.DeviceIdType.MESH,
        )

    peer = dev(dc=1)

    def go(cp):
        cp.start()
        return cp

    def arrived(ref, sem):
        remote(ref, ref, sem, sem, peer).wait_recv()

    def gone(ref, sem):
        remote(ref, ref, sem, sem, peer).wait_send()

    (S_KV, S_Q, S_DK, S_DQ, S_O, S_A, S_WO, S_P, S_WU, S_SQ, S_IV, S_N, S_ND, S_X, S_AD, S_F,
     S_C) = [out_s.at[i] for i in range(17)]
    R_DK, R_DQ, R_A, R_WO, R_WU, R_WP, R_SQ, R_IV, R_F, R_C, R_WL = [
        one_r.at[i] for i in range(11)
    ]

    def lane(ref, h):
        return ref.at[:, h * HEAD_DIM : (h + 1) * HEAD_DIM]

    for h in range(HEADS):
        pltpu.make_async_copy(lane(k_ref, h), kvb.at[0, h, 0], own_l.at[0]).start()
        pltpu.make_async_copy(lane(v_ref, h), kvb.at[0, h, 1], own_l.at[0]).start()
        pltpu.make_async_copy(lane(q_ref, h), qb.at[0, h], own_l.at[1]).start()
    big = [
        pltpu.make_async_copy(win_ref, wi_own, l_s.at[0]),
        pltpu.make_async_copy(wout_ref, wo_own, l_s.at[1]),
        pltpu.make_async_copy(resid_ref, res, l_s.at[2]),
    ]
    for cp in big:
        cp.start()

    barrier = pltpu.get_barrier_semaphore()
    friends = [peer]
    for r in (1, 2, 3):
        friends += [dev(dy=r), dev(dy=r, dc=1), dev(dz=r), dev(dx=r), dev(dx=r, dc=1)]
    for f in friends:
        pl.semaphore_signal(barrier, inc=1, device_id=f, device_id_type=pl.DeviceIdType.MESH)
    doc_here = jnp.broadcast_to(doc_ref[...].astype(F32), (8, TOK))
    drow[0] = doc_here
    qrow[0] = doc_here
    pl.semaphore_wait(barrier, len(friends))
    for r in (1, 2, 3):
        go(remote(drow.at[0], drow.at[r], S_DK, R_DK, dev(dy=r)))
    for r in (1, 2):
        go(remote(drow.at[0], qrow.at[r], S_DQ, R_DQ, dev(dz=-r)))
    pltpu.make_async_copy(kvb.at[0], kvb.at[0], own_l.at[0]).wait()
    pltpu.make_async_copy(qb.at[0], qb.at[0], own_l.at[1]).wait()

    def direct(h):
        return [
            remote(kvb.at[0, h], kvb.at[r, h], S_KV, kv_r.at[r // 2, h], dev(dy=r)) for r in (1, 3)
        ]

    def relay(h):
        return [
            remote(kvb.at[1, h, 0], kvb.at[2, h, 0], S_KV, kv_r.at[2, h], dev(dy=1)),
            remote(kvb.at[3, h, 1], kvb.at[2, h, 1], S_KV, kv_r.at[2, h], dev(dy=3)),
        ]

    def ask(h):
        return [remote(qb.at[0, h], qb.at[r, h], S_Q, q_r.at[h], dev(dz=-r)) for r in (1, 2)]

    for h in range(HEADS):
        if h < 2:
            for cp in direct(h):
                cp.start()
        for r, cp in zip((1, 2), ask(h)):
            pl.when(z >= r)(cp.start)

    rows_c = pl.ds(pl.multiple_of(c * WID, 128), WID)

    def chunk(of):
        return oproj_ref.at[:, pl.ds(pl.multiple_of(of * WID, 128), WID)]

    rows_o = pl.ds(pl.multiple_of((1 - c) * WID, 128), WID)
    wo_loc = [
        pltpu.make_async_copy(chunk(2 * d + c), wo.at[d, rows_c, :], R_WL) for d in range(4)
    ]
    wo_rem = [
        remote(chunk(2 * d + 1 - c), wo.at[d, rows_c, :], S_WO, R_WO, peer) for d in range(4)
    ]

    ct = y // 2
    left, right = (y + 3) % 4, (y + 1) % 4

    def hot_cols(g):
        return pl.ds(pl.multiple_of((g % 2) * SLOTS, 128), SLOTS)

    win_dst = win.at[rows_c, hot_cols(y)]
    my_rows = pl.ds(pl.multiple_of(y * SLOTS, 128), SLOTS)
    wi_peer = remote(hin, win_dst, wi_s.at[0], wi_r.at[y % 2, c], peer)

    def choose():
        for cp in big:
            cp.wait()
        live = lax.broadcasted_iota(jnp.int32, (1, SLOTS), 1) < BLOCK * hblk_ref[0]
        want = jnp.where(live, hidx_ref[...], -1)
        pick = (lax.broadcasted_iota(jnp.int32, (NEUR, SLOTS), 0) == want).astype(F32).astype(BF)
        hin[...] = dot(wi_own[...], pick, ((0,), (0,))).astype(BF)
        wou[my_rows, :] = dot(pick, wo_own[...], ((0,), (0,))).astype(BF)

        @pl.when(ct == c)
        def _():
            win[rows_c, hot_cols(y)] = hin[...]

        @pl.when(ct != c)
        def _():
            wi_peer.start()

    wi_out = [
        remote(hin, win_dst, wi_s.at[r], wi_r.at[y % 2, c], (z * 4 + (y + r) % 4, 2 * x + ct))
        for r in (1, 3)
    ]
    wu_out = [
        remote(wou.at[my_rows], wou.at[my_rows], S_WU, R_WU, dev(dy=r)) for r in (1, 3)
    ]

    def pass_in(j):
        g = (left, right)[j]
        part = win.at[j * WID : (j + 1) * WID, hot_cols(g)]
        return g // 2 == c, remote(
            part, part, wi_s.at[4 + j], wi_r.at[g % 2, j], dev(dy=(1, 3)[j])
        )

    def pass_out(j):
        g = (left, right)[j]
        part = wou.at[pl.ds(pl.multiple_of(g * SLOTS + j * (SLOTS // 2), 64), SLOTS // 2)]
        return remote(part, part, S_WU, R_WP, dev(dy=(1, 3)[j]))

    def both(top, total):
        row = lax.broadcasted_iota(jnp.int32, (8, TOK), 0)
        return jnp.where(row == 0, top, total)

    for i in (1, 2):

        @pl.when(z < i)
        def _():
            orecv[i - 1] = jnp.zeros_like(orecv[i - 1])
            srecv[i - 1] = jnp.broadcast_to(
                both(jnp.full((1, TOK), LOW, F32), jnp.zeros((1, TOK), F32)), (HEADS, 8, TOK)
            )

    choose()
    arrived(drow.at[1:4], R_DK)
    arrived(qrow.at[1:3], R_DQ)
    for r in range(4):
        kcol[r] = jnp.transpose(jnp.broadcast_to(drow[r][0:1, :], (128, TOK)))

    def pair(h, i, r, qd, causal=False):
        sc = dot(kvb[r, h, 0], qb[i, h], ((1,), (1,)))
        kd = kcol[r]
        mask = jnp.concatenate([kd, kd], axis=1) == qd
        if causal:
            key_at = lax.broadcasted_iota(jnp.int32, (TOK, TOK), 0)
            query_at = lax.broadcasted_iota(jnp.int32, (TOK, TOK), 1)
            mask = mask & (key_at <= query_at)
        sc = jnp.where(mask, sc, MASKED)
        top = jnp.maximum(jnp.max(sc, axis=0, keepdims=True), LOW)
        p = jnp.exp2((sc - top) * SCALE2)
        total = jnp.sum(p, axis=0, keepdims=True)
        return top, total, dot(kvb[r, h, 1], p.astype(BF), ((0,), (0,)))

    def together(results):
        top = results[0][0]
        for other, _, _ in results[1:]:
            top = jnp.maximum(top, other)
        total, acc = 0.0, 0.0
        for own, part, mixed in results:
            factor = jnp.exp2((own - top) * SCALE2)
            total = total + part * factor
            acc = acc + mixed * factor
        return top, total, acc

    def back(i, h):
        return (
            remote(
                osend.at[i - 1, h, 0:128], orecv.at[i - 1, h, 0:128], S_O, o_r.at[h],
                (((z + i) % 4) * 4 + y, m),
            ),
            remote(
                ssend.at[i - 1, h], srecv.at[i - 1, h], S_O, o_r.at[h],
                (((z + i) % 4) * 4 + y, m),
            ),
        )

    def head(h, _):
        @pl.when(h + 2 < HEADS)
        def _():
            for cp in direct(h + 2):
                cp.start()

        @pl.when(z <= 1)
        def _():
            arrived(qb.at[1:3, h], q_r.at[h])

        @pl.when(z == 2)
        def _():
            arrived(qb.at[1, h], q_r.at[h])

        q0 = qrow[0][0:1, :]
        q1 = jnp.where(z + 1 <= 3, qrow[1][0:1, :], -5.0)
        q2 = jnp.where(z + 2 <= 3, qrow[2][0:1, :], -5.0)

        def shared(n):
            if n == 0:
                return pair(h, 0, 0, q0, True)
            own = n <= y
            slot = jnp.where(own, n, jnp.where(n == y + 1, 0, n - 1))
            return pair(h, jnp.where(own, 0, 2), slot, jnp.where(own, q0, q2))

        near, mix = {}, {}
        for n in (0, 1, 3):
            near[n] = pair(h, 1, n, q1)
        for n in (0, 1, 4):
            mix[n] = shared(n)

        @pl.when(h + 1 < HEADS)
        def _():
            pass_on(h + 1)

        @pl.when(h == HEADS - 2)
        def _():
            for cp in wi_out:
                cp.start()

        arrived(kvb.at[2, h], kv_r.at[2, h])
        for n in (2, 3):
            mix[n] = shared(n)
        far = [
            (jnp.where(n <= y, LOW, mix[n][0]), mix[n][1], mix[n][2]) for n in (1, 2, 3)
        ] + [mix[4]]
        for i, parts_of in ((2, far), (1, None)):
            if i == 1:
                near[2] = pair(h, 1, 2, q1)
                parts_of = [near[n] for n in range(4)]
            top, total, acc = together(parts_of)
            osend[i - 1, h, 0:128] = acc.astype(BF)
            ssend[i - 1, h] = both(top, total)

            @pl.when(z + i <= 3)
            def _():
                for cp in back(i, h):
                    cp.start()

        top, total, acc = together(
            [mix[0]] + [(jnp.where(n <= y, mix[n][0], LOW), mix[n][1], mix[n][2]) for n in (1, 2, 3)]
        )
        acc0[h] = acc
        st0[h] = both(top, total)

        @pl.when(h == 0)
        def _():
            for cp in wo_loc + wo_rem:
                cp.start()

        return 0

    def pass_on(h):
        for cp in direct(h):
            cp.wait_recv()
        for cp in relay(h):
            cp.start()

    pass_on(0)
    lax.fori_loop(0, HEADS, head, 0)

    def swap(h):
        return remote(att.at[c, h], att.at[c, h], S_A, R_A, peer)

    def merge(h, _):
        @pl.when(z >= 2)
        def _():
            arrived(orecv.at[:, h], o_r.at[h])

        @pl.when(z == 1)
        def _():
            arrived(orecv.at[0, h], o_r.at[h])

        t0, t1, t2 = st0[h][0:1, :], srecv[0, h][0:1, :], srecv[1, h][0:1, :]
        n0, n1, n2 = st0[h][1:2, :], srecv[0, h][1:2, :], srecv[1, h][1:2, :]
        top = jnp.maximum(t0, jnp.maximum(t1, t2))
        f0 = jnp.exp2((t0 - top) * SCALE2)
        f1 = jnp.exp2((t1 - top) * SCALE2)
        f2 = jnp.exp2((t2 - top) * SCALE2)
        inv = 1.0 / (n0 * f0 + n1 * f1 + n2 * f2)
        mixed = (
            acc0[h] * (f0 * inv)
            + orecv[0, h, 0:128].astype(F32) * (f1 * inv)
            + orecv[1, h, 0:128].astype(F32) * (f2 * inv)
        )
        att[c, h] = jnp.transpose(mixed).astype(BF)
        swap(h).start()
        return 0

    lax.fori_loop(0, HEADS, merge, 0)

    pltpu.make_async_copy(wo.at[:, rows_c, :], wo.at[:, rows_c, :], R_WL).wait()
    arrived(wo.at[:, rows_o, :], R_WO)
    arrived(att.at[1 - c], R_A)
    both_att = jnp.concatenate([att[i, h] for i in (0, 1) for h in range(HEADS)], axis=1)

    def span(k, j):
        return slice(128 * k + 64 * j, 128 * k + 64 * j + 64)

    def project(dx, k):
        return dot(both_att[128 * k : 128 * k + 128], wo[(x + dx) % 4], ((1,), (0,)))

    def across(k):
        psend[2, 128 * k : 128 * k + 128] = project(2, k).astype(BF)
        for j, e in ((0, 1), (1, 3)):
            go(remote(psend.at[2, span(k, j)], prel.at[k, j], S_P, p_r.at[k], dev(dx=e)))

    def beside(k):
        for j, e in ((0, 1), (1, 3)):
            pnear[j, 128 * k : 128 * k + 128] = project(e, k)
            rows = span(k, 1 - j)
            psend[e, rows] = pnear[j, rows].astype(BF)
            half = slice(64 - 64 * j, 128 - 64 * j)
            go(remote(psend.at[e, rows], precv.at[k, j, half], S_P, p_r.at[2 + k], dev(dx=e)))

    def onward(k):
        arrived(prel.at[k], p_r.at[k])
        for j, e in ((0, 1), (1, 3)):
            rows = span(k, j)
            psend[e, rows] = (pnear[j, rows] + prel[k, j].astype(F32)).astype(BF)
            half = slice(64 * j, 64 * j + 64)
            go(remote(psend.at[e, rows], precv.at[k, j, half], S_P, p_r.at[2 + k], dev(dx=e)))

    across(0)
    beside(0)
    across(1)

    for j in (0, 1):
        here, cp = pass_in(j)

        @pl.when(here)
        def _():
            cp.wait_recv()
            cp.start()

    onward(0)
    beside(1)
    for k in (0, 1):
        at = slice(128 * k, 128 * k + 128)
        fown[at] = project(0, k) + res[at].astype(F32)
    onward(1)

    n_in, nd_in = {}, {}

    def tokens(r, k):
        half = slice(128 * k, 128 * k + 128)
        n_in[r, k] = go(
            remote(nb.at[0, c, half], nb.at[r, c, half], S_N, n_r.at[r - 1, k], dev(dz=r))
        )

    def mate(r, k):
        half = nb.at[r, c, 128 * k : 128 * k + 128]
        nd_in[r, k] = go(remote(half, half, S_ND, nd_r.at[r, k], peer))

    gain = gain_ref[...].astype(F32).reshape(1, WID)

    def settle(k):
        at = slice(128 * k, 128 * k + 128)
        arrived(precv.at[k], p_r.at[2 + k])
        state = (fown[at] + precv[k, 0].astype(F32) + precv[k, 1].astype(F32)).astype(BF)
        res[at] = state
        nb[0, c, at] = (state.astype(F32) * gain).astype(BF)
        mate(0, k)

    settle(0)
    for r in (1, 3):
        tokens(r, 0)

    def stage_w(b):
        arrived(wou.at[0 : 2 * SLOTS], R_WU)
        for j in (0, 1):
            go(pass_out(j))

    for gi in (0, 1):
        for cs in (0, 1):
            g = 2 * c + gi
            had = jnp.logical_or(
                jnp.logical_and(g == y, c == cs), g == (left, right)[cs]
            )

            @pl.when(jnp.logical_not(had))
            def _():
                remote(hin, win_dst, wi_s.at[0], wi_r.at[gi, cs], peer).wait_recv()

    csum[...] = jnp.zeros_like(csum)
    parts = tuple(
        (r, 128 * k, 128)
        for r, k in ((0, 0), (0, 1), (1, 0), (3, 0), (2, 0), (2, 1), (1, 1), (3, 1))
    )

    plain = ()

    def quarter(b, at):
        _, first, n = parts[b]
        return pl.ds(pl.multiple_of(first + at * (n // 4), 32), n // 4)

    def eighth(b, at, j):
        _, first, n = parts[b]
        return pl.ds(pl.multiple_of(first + at * (n // 4) + j * (n // 8), 16), n // 8)

    def columns_of(r, row):
        inv_col[r] = jnp.transpose(jnp.broadcast_to(row, (128, TOK)))

    def stage_n(b):
        arrived(sqs.at[1:8], R_SQ)
        squares = sqs[0]
        for j in range(1, 8):
            squares = squares + sqs[j]
        inv_row[0] = lax.rsqrt(squares / D + EPS)
        for r in ORDER:
            go(remote(inv_row.at[0], inv_row.at[r], S_IV, R_IV, dev(dz=r)))
        columns_of(0, inv_row[0][0:1, :])

    def stage_a(b):
        r, first, n = parts[b]
        k = first // 128
        arrived(nb.at[r, c, first : first + n], n_r.at[r - 1, k])
        mate(r, k)
        if r != 2:
            half = slice(first + 32 * (r - 1), first + 32 * (r - 1) + 64)
            go(remote(nb.at[r, c, half], nb.at[2, c, half], S_N, n_r.at[1, k], dev(dz=r)))

    def stage_b(b):
        r, first, n = parts[b]
        nd_in[r, first // 128].wait_recv()
        at = slice(first, first + n)
        rows = jnp.concatenate([nb[r, 0, at], nb[r, 1, at]], axis=1)
        pre = dot(rows, win[...], ((1,), (0,)))
        prebuf[r, at] = pre
        presend[r, at] = pre.astype(BF)
        h = n // 8
        if b in plain:
            for e in (2, 1, 3):
                go(
                    remote(
                        presend.at[r, quarter(b, (x + e) % 4)], prerecv.at[b, e - 1], S_X,
                        rs_r.at[b], dev(dx=e),
                    )
                )
            return
        for j, e in ((0, 1), (1, 3)):
            rest = slice(h - j * h, 2 * h - j * h)
            go(
                remote(
                    presend.at[r, eighth(b, (x + 2) % 4, j)], relrecv.at[b, j], S_X, rel_r.at[b],
                    dev(dx=e),
                )
            )
            go(
                remote(
                    presend.at[r, eighth(b, (x + e) % 4, 1 - j)], prerecv.at[b, j, rest], S_X,
                    rs_r.at[b], dev(dx=e),
                )
            )

    def stage_r(b):
        r, first, n = parts[b]
        h = n // 8
        arrived(relrecv.at[b], rel_r.at[b])
        for j, e in ((0, 1), (1, 3)):
            half = slice(j * h, j * h + h)
            there = eighth(b, (x + e) % 4, j)
            relsend[b, j] = (
                prebuf[r, there, :] + relrecv[b, j].astype(F32)
            ).astype(BF)
            go(remote(relsend.at[b, j], prerecv.at[b, j, half], S_X, rs_r.at[b], dev(dx=e)))

    def stage_c(b):
        r, first, n = parts[b]
        arrived(prerecv.at[b, 0 : 3 if b in plain else 2], rs_r.at[b])
        if b == 2:
            arrived(inv_row.at[1:4], R_IV)
        if r and first == 0:
            columns_of(r, inv_row[r][0:1, :])
        here = quarter(b, x)
        q = slice(0, n // 4)
        pre = (
            prebuf[r, here, :] + prerecv[b, 0, q].astype(F32) + prerecv[b, 1, q].astype(F32)
        )
        if b in plain:
            pre = pre + prerecv[b, 2].astype(F32)
        factor = inv_col[r, here, :]
        active = jnp.maximum(pre, 0.0) * jnp.concatenate([factor] * 6, axis=1)
        csum[...] += jnp.sum(active, axis=0, keepdims=True)
        ab[r, c, here, :] = active.astype(BF)
        for e in (2, 1, 3) if b in plain else (1, 3):
            go(remote(ab.at[r, c, here], ab.at[r, c, here], S_X, ag_r.at[b], dev(dx=e)))

    def stage_d(b):
        r, first, n = parts[b]
        arrived(ab.at[r, c, first : first + n // 2], ag_r.at[b])
        for j, e in ((0, 1), (1, 3)):
            block = ab.at[r, c, eighth(b, (x - e) % 4, j)]
            go(remote(block, block, S_X, fwd_r.at[b], dev(dx=e)))

    def stage_g(b):
        r, first, n = parts[b]
        if b in plain:
            arrived(ab.at[r, c, first : first + 3 * n // 4], ag_r.at[b])
        else:
            arrived(ab.at[r, c, first : first + n // 4], fwd_r.at[b])
        block = ab.at[r, c, first : first + n]
        go(remote(block, block, S_AD, ad_r.at[b], peer))

    def stage_e(b):
        r, first, n = parts[b]
        if b == 0:
            arrived(wou.at[0:SLOTS], R_WP)
        arrived(ab.at[r, 1 - c, first : first + n], ad_r.at[b])
        at = slice(first, first + n)
        rows = jnp.concatenate([ab[r, 0, at], ab[r, 1, at]], axis=1)
        part = dot(rows, wou[...], ((1,), (0,)))
        if r == 0:
            fown[at] = part + res[at].astype(F32)
        else:
            k = first // 128
            for j, e in ((0, 3), (1, 1)):
                mine = slice(64 * j, 64 * j + 64)
                there = slice(first + 64 * j, first + 64 * j + 64)
                if r == 2:
                    fsend[r, there] = part[mine].astype(BF)
                    go(remote(fsend.at[r, there], frel.at[k, j], S_F, fr_r.at[k, j], dev(dz=e)))
                elif r == e:
                    fsend[r, there] = part[mine].astype(BF)
                    home(r, there)
                else:
                    fpart[k, j] = part[mine]

    def home(r, rows):
        go(remote(fsend.at[r, rows], frecv.at[r // 2, rows], S_F, R_F, dev(dz=-r)))

    def stage_q(b):
        r, first, n = parts[b]
        k, j = first // 128, r // 2
        arrived(frel.at[k, j], fr_r.at[k, j])
        rows = slice(first + 64 * j, first + 64 * j + 64)
        fsend[r, rows] = (fpart[k, j] + frel[k, j].astype(F32)).astype(BF)
        home(r, rows)

    def stage_s(b):
        for cp in wu_out:
            cp.start()
        settle(1)
        wide = res[...].astype(F32)
        square = wide * wide
        high = square.astype(BF)
        rest = (square - high.astype(F32)).astype(BF)
        ones = jnp.ones((8, WID), BF)
        sqs[0] = dot(ones, high, ((1,), (1,))) + dot(ones, rest, ((1,), (1,)))
        for j in range(1, 8):
            go(remote(sqs.at[0], sqs.at[j], S_SQ, R_SQ, dev(dx=j // 2, dc=j % 2)))

    def stage_t(b):
        tokens(parts[b][0], parts[b][1] // 128)

    def stage_h(b):
        for r in (1, 2, 3):
            go(remote(csum, csr.at[r], S_C, R_C, dev(dx=r)))

    stage = {
        "n": stage_n, "a": stage_a, "b": stage_b, "r": stage_r, "c": stage_c, "d": stage_d,
        "g": stage_g, "e": stage_e, "h": stage_h, "s": stage_s, "t": stage_t, "w": stage_w,
        "q": stage_q,
    }
    for word in PLAN:
        stage[word[0]](int(word[1]))

    arrived(csr.at[1:4], R_C)
    sums = csum[...] + csr[1] + csr[2] + csr[3]
    h_out = []
    for gi in (0, 1):
        hs[gi] = sums[:, gi * SLOTS : (gi + 1) * SLOTS]
    for gi in (0, 1):
        for cd in (0, 1):
            cp = remote(
                hs.at[gi], hsr.at[y], h_s.at[gi, cd], h_r.at[y],
                (z * 4 + 2 * c + gi, 2 * x + cd),
            )
            mine = jnp.logical_and(y == 2 * c + gi, c == cd)
            h_out.append((cp, mine))

            @pl.when(jnp.logical_not(mine))
            def _():
                cp.start()

            @pl.when(mine)
            def _():
                hsr[y] = hs[gi]

    arrived(frecv, R_F)
    out_ref[...] = (
        fown[...] + frecv[0].astype(F32) + frecv[1].astype(F32)
    ).astype(BF)

    for src in range(4):
        @pl.when(jnp.logical_not(jnp.logical_and(src == y, y // 2 == c)))
        def _():
            remote(hs.at[0], hsr.at[src], h_s.at[0, 0], h_r.at[src], peer).wait_recv()

    hm_ref[...] = (hsr[0] + hsr[1] + hsr[2] + hsr[3])[0:1, :] / TOKENS

    gone(kvb.at[0:3], S_KV)
    @pl.when(z >= 2)
    def _():
        gone(qb.at[0:2], S_Q)

    @pl.when(z == 1)
    def _():
        gone(qb.at[0], S_Q)

    @pl.when(z <= 1)
    def _():
        gone(orecv, S_O)

    @pl.when(z == 2)
    def _():
        gone(orecv.at[0], S_O)

    gone(drow.at[0:3], S_DK)
    gone(drow.at[0:2], S_DQ)
    gone(att.at[c], S_A)
    gone(wo.at[:, rows_c, :], S_WO)
    gone(psend.at[0:3], S_P)
    gone(wou.at[0 : 3 * SLOTS], S_WU)
    gone(sqs.at[1:8], S_SQ)
    gone(inv_row.at[1:4], S_IV)
    gone(fsend.at[1:4], S_N)
    gone(nb.at[0:2], S_ND)
    gone(ab.at[0:3], S_X)
    gone(presend, S_AD)
    gone(fsend.at[1:4], S_F)
    gone(csr.at[1:4], S_C)
    for cp, mine in h_out:
        @pl.when(jnp.logical_not(mine))
        def _():
            cp.wait_send()

    @pl.when(ct != c)
    def _():
        wi_peer.wait_send()

    for cp in wi_out:
        cp.wait_send()
    for j in (0, 1):
        here, cp = pass_in(j)

        @pl.when(here)
        def _():
            cp.wait_send()


def finish(layer_ref, mean_ref, out_ref, hm_ref):
    out_ref[...] = layer_ref[...]
    hm_ref[...] = mean_ref[...]


def local(resid, queries, keys, values, doc_ids, out_proj, ffn_gain, w_in, w_out, hot_index,
          hot_blocks):
    dma = pltpu.SemaphoreType.DMA
    V = pltpu.VMEM
    hbm = pl.BlockSpec(memory_space=pl.ANY)
    vm = pl.BlockSpec(memory_space=pltpu.VMEM)
    sm = pl.BlockSpec(memory_space=pltpu.SMEM)
    scratch = [
        V((3, HEADS, TOK, 128), BF), V((4, HEADS, 2, TOK, 128), BF),
        V((4, 8, TOK), F32), V((3, 8, TOK), F32), V((4, TOK, 128), F32),
        V((HEADS, 128, TOK), F32), V((HEADS, 8, TOK), F32),
        V((2, HEADS, 144, TOK), BF), V((2, HEADS, 8, TOK), F32),
        V((2, HEADS, 144, TOK), BF), V((2, HEADS, 8, TOK), F32),
        V((2, HEADS, TOK, 128), BF), V((4, 2 * WID, WID), BF), V((TOK, WID), BF),
        V((4, TOK, WID), BF), V((2, 2, 128, WID), BF), V((2, 2, 64, WID), BF), V((2, TOK, WID), F32),
        V((NEUR, WID), BF), V((NEUR, WID), BF), V((WID, SLOTS), BF),
        V((2 * WID, 2 * SLOTS), BF), V((4 * SLOTS, WID), BF),
        V((8, 8, TOK), F32), V((4, 8, TOK), F32), V((4, TOK, 128), F32), V((4, 2, TOK, WID), BF),
        V((4, TOK, 2 * SLOTS), F32),
        V((4, TOK, 2 * SLOTS), BF), V((8, 3, 32, 2 * SLOTS), BF), V((8, 2, 16, 2 * SLOTS), BF),
        V((8, 2, 16, 2 * SLOTS), BF), V((4, 2, TOK, 2 * SLOTS), BF),
        V((TOK, WID), F32), V((4, TOK, WID), BF), V((2, TOK, WID), BF), V((2, 2, 64, WID), BF),
        V((2, 2, 64, WID), F32),
        V((8, 2 * SLOTS), F32), V((4, 8, 2 * SLOTS), F32), V((2, 8, SLOTS), F32),
        V((4, 8, SLOTS), F32),
        dma((17,)), dma((3, HEADS)), dma((HEADS,)), dma((HEADS,)), dma((4,)), dma((3,)), dma((2,)),
        dma((6,)), dma((2, 2)), dma((3, 2)), dma((4, 2)), dma((8,)), dma((8,)), dma((8,)),
        dma((8,)), dma((8,)), dma((2, 2)), dma((11,)), dma((2, 2)), dma((4,)),
    ]
    layer, mean = pl.pallas_call(
        kernel,
        out_shape=(
            jax.ShapeDtypeStruct((TOK, WID), BF), jax.ShapeDtypeStruct((1, SLOTS), F32),
        ),
        in_specs=[hbm, hbm, hbm, hbm, vm, hbm, vm, hbm, hbm, vm, sm],
        out_specs=(vm, vm),
        scratch_shapes=scratch,
        compiler_params=pltpu.CompilerParams(
            collective_id=0, has_side_effects=True, vmem_limit_bytes=60 * 2**20
        ),
        name="layer",
    )(
        queries, keys, values, resid, doc_ids.reshape(1, TOK), out_proj,
        ffn_gain, w_in.T, w_out, hot_index, hot_blocks,
    )
    return pl.pallas_call(
        finish, out_shape=(
            jax.ShapeDtypeStruct((TOK, WID), BF), jax.ShapeDtypeStruct((1, SLOTS), F32),
        ), in_specs=[vm, vm], out_specs=(vm, vm), name="finish",
    )(layer, mean)


def solution(mesh):
    return jax.shard_map(
        local,
        mesh=mesh,
        in_specs=(
            P("seq", "mp"), P("seq", "mp"), P("seq", "mp"), P("seq", "mp"), P("seq"),
            P("mp", None), P("mp"), P("mp", "seq"), P("seq", "mp"), P("seq", None), P("seq"),
        ),
        out_specs=(P("seq", "mp"), P("seq", None)),
        check_vma=False,
    )
```

```python
import jax
import jax.numpy as jnp
from jax import lax
from jax.experimental import pallas as pl
from jax.experimental.pallas import tpu as pltpu
from jax.sharding import PartitionSpec as P

HEAD_DIM = 128
HEADS = 5
TOK = 256
WID = 640
SLOTS = 384
BLOCK = 128
NEUR = 864
D = 5120
TOKENS = 4096
EPS = 1e-05
LOW = -1e9
MASKED = -2e9
SCALE2 = HEAD_DIM ** (-0.5) * 1.4426950408889634
BF = jnp.bfloat16
F32 = jnp.float32
ORDER = (1, 3, 2)
PLAN = (
    "b0", "s0", "t7", "t6", "r0", "a2", "a3", "b1", "n0", "c0", "b2", "b3", "r1", "a7", "a6",
    "d0", "a4", "r2", "b4", "r3", "b6", "c1", "g0", "a5", "c2", "r4", "b5", "w0", "c3", "d1",
    "r6", "b7", "d2", "c4", "r5", "d3", "g1", "c6", "e0", "e1", "g2", "r7", "d4", "c5", "g3",
    "e2", "d6", "c7", "h0", "e3", "g4", "d5", "g6", "e4", "d7", "e6", "g5", "q2", "e5", "q3",
    "g7", "e7", "q6", "q7",
)


def dot(a, b, dims):
    return lax.dot_general(a, b, (dims, ((), ())), preferred_element_type=F32)


def kernel(
    q_ref, k_ref, v_ref, resid_ref, doc_ref, oproj_ref, gain_ref, win_ref, wout_ref, hidx_ref,
    hblk_ref, out_ref, hm_ref,
    doc_here, gain_here, hidx_here, qb, kvb, drow, qrow, kcol, acc0, st0, osend, ssend, orecv, srecv, att, wo, res,
    psend, precv, prel, pnear, wi_own, wo_own, hin, win, wou, sqs, inv_row, inv_col, nb, prebuf,
    presend, prerecv, relrecv, relsend, ab, fown, fsend, frecv, frel, fpart, csum, csr, hs, hsr,
    out_s, kv_r, q_r, o_r, p_r, l_s, own_l, wi_s, wi_r, n_r, nd_r, rel_r, rs_r, ag_r, fwd_r, ad_r,
    fr_r, one_r, h_s, h_r,
):
    s = lax.axis_index("seq")
    m = lax.axis_index("mp")
    z, y, x, c = s // 4, s % 4, m // 2, m % 2

    def dev(dz=0, dy=0, dx=0, dc=0):
        return (((z + dz) % 4) * 4 + (y + dy) % 4, ((x + dx) % 4) * 2 + (c + dc) % 2)

    def remote(src, dst, ss, rs, device):
        return pltpu.make_async_remote_copy(
            src_ref=src, dst_ref=dst, send_sem=ss, recv_sem=rs, device_id=device,
            device_id_type=pl.DeviceIdType.MESH,
        )

    peer = dev(dc=1)

    def go(cp):
        cp.start()
        return cp

    def arrived(ref, sem):
        remote(ref, ref, sem, sem, peer).wait_recv()

    def gone(ref, sem):
        remote(ref, ref, sem, sem, peer).wait_send()

    (S_KV, S_Q, S_DK, S_DQ, S_O, S_A, S_WO, S_P, S_WU, S_SQ, S_IV, S_N, S_ND, S_X, S_AD, S_F,
     S_C) = [out_s.at[i] for i in range(17)]
    R_DK, R_DQ, R_A, R_WO, R_WU, R_WP, R_SQ, R_IV, R_F, R_C, R_WL = [
        one_r.at[i] for i in range(11)
    ]

    def lane(ref, h):
        return ref.at[:, h * HEAD_DIM : (h + 1) * HEAD_DIM]

    for h in range(HEADS):
        pltpu.make_async_copy(lane(k_ref, h), kvb.at[0, h, 0], own_l.at[0]).start()
        pltpu.make_async_copy(lane(v_ref, h), kvb.at[0, h, 1], own_l.at[0]).start()
        pltpu.make_async_copy(lane(q_ref, h), qb.at[0, h], own_l.at[1]).start()
    big = [
        pltpu.make_async_copy(win_ref, wi_own, l_s.at[0]),
        pltpu.make_async_copy(wout_ref, wo_own, l_s.at[1]),
        pltpu.make_async_copy(resid_ref, res, l_s.at[2]),
    ]
    small = [
        pltpu.make_async_copy(doc_ref, doc_here, l_s.at[3]),
        pltpu.make_async_copy(gain_ref, gain_here, l_s.at[4]),
        pltpu.make_async_copy(hidx_ref, hidx_here, l_s.at[5]),
    ]
    for cp in small + big:
        cp.start()

    barrier = pltpu.get_barrier_semaphore()
    friends = [peer]
    for r in (1, 2, 3):
        friends += [dev(dy=r), dev(dy=r, dc=1), dev(dz=r), dev(dx=r), dev(dx=r, dc=1)]
    for f in friends:
        pl.semaphore_signal(barrier, inc=1, device_id=f, device_id_type=pl.DeviceIdType.MESH)
    for cp in small:
        cp.wait()
    documents = jnp.broadcast_to(doc_here[...].astype(F32), (8, TOK))
    drow[0] = documents
    qrow[0] = documents
    pl.semaphore_wait(barrier, len(friends))
    for r in (1, 2, 3):
        go(remote(drow.at[0], drow.at[r], S_DK, R_DK, dev(dy=r)))
    for r in (1, 2):
        go(remote(drow.at[0], qrow.at[r], S_DQ, R_DQ, dev(dz=-r)))
    pltpu.make_async_copy(kvb.at[0], kvb.at[0], own_l.at[0]).wait()
    pltpu.make_async_copy(qb.at[0], qb.at[0], own_l.at[1]).wait()

    def direct(h):
        return [
            remote(kvb.at[0, h], kvb.at[r, h], S_KV, kv_r.at[r // 2, h], dev(dy=r)) for r in (1, 3)
        ]

    def relay(h):
        return [
            remote(kvb.at[1, h, 0], kvb.at[2, h, 0], S_KV, kv_r.at[2, h], dev(dy=1)),
            remote(kvb.at[3, h, 1], kvb.at[2, h, 1], S_KV, kv_r.at[2, h], dev(dy=3)),
        ]

    def ask(h):
        return [remote(qb.at[0, h], qb.at[r, h], S_Q, q_r.at[h], dev(dz=-r)) for r in (1, 2)]

    for h in range(HEADS):
        if h < 2:
            for cp in direct(h):
                cp.start()
        for r, cp in zip((1, 2), ask(h)):
            pl.when(z >= r)(cp.start)

    rows_c = pl.ds(pl.multiple_of(c * WID, 128), WID)

    def chunk(of):
        return oproj_ref.at[:, pl.ds(pl.multiple_of(of * WID, 128), WID)]

    rows_o = pl.ds(pl.multiple_of((1 - c) * WID, 128), WID)
    wo_loc = [
        pltpu.make_async_copy(chunk(2 * d + c), wo.at[d, rows_c, :], R_WL) for d in range(4)
    ]
    wo_rem = [
        remote(chunk(2 * d + 1 - c), wo.at[d, rows_c, :], S_WO, R_WO, peer) for d in range(4)
    ]

    ct = y // 2
    left, right = (y + 3) % 4, (y + 1) % 4

    def hot_cols(g):
        return pl.ds(pl.multiple_of((g % 2) * SLOTS, 128), SLOTS)

    win_dst = win.at[rows_c, hot_cols(y)]
    my_rows = pl.ds(pl.multiple_of(y * SLOTS, 128), SLOTS)
    wi_peer = remote(hin, win_dst, wi_s.at[0], wi_r.at[y % 2, c], peer)

    def choose():
        for cp in big:
            cp.wait()
        live = lax.broadcasted_iota(jnp.int32, (1, SLOTS), 1) < BLOCK * hblk_ref[0]
        want = jnp.where(live, hidx_here[...], -1)
        pick = (lax.broadcasted_iota(jnp.int32, (NEUR, SLOTS), 0) == want).astype(F32).astype(BF)
        hin[...] = dot(wi_own[...], pick, ((0,), (0,))).astype(BF)
        wou[my_rows, :] = dot(pick, wo_own[...], ((0,), (0,))).astype(BF)

        @pl.when(ct == c)
        def _():
            win[rows_c, hot_cols(y)] = hin[...]

        @pl.when(ct != c)
        def _():
            wi_peer.start()

    wi_out = [
        remote(hin, win_dst, wi_s.at[r], wi_r.at[y % 2, c], (z * 4 + (y + r) % 4, 2 * x + ct))
        for r in (1, 3)
    ]
    wu_out = [
        remote(wou.at[my_rows], wou.at[my_rows], S_WU, R_WU, dev(dy=r)) for r in (1, 3)
    ]

    def pass_in(j):
        g = (left, right)[j]
        part = win.at[j * WID : (j + 1) * WID, hot_cols(g)]
        return g // 2 == c, remote(
            part, part, wi_s.at[4 + j], wi_r.at[g % 2, j], dev(dy=(1, 3)[j])
        )

    def pass_out(j):
        g = (left, right)[j]
        part = wou.at[pl.ds(pl.multiple_of(g * SLOTS + j * (SLOTS // 2), 64), SLOTS // 2)]
        return remote(part, part, S_WU, R_WP, dev(dy=(1, 3)[j]))

    def both(top, total):
        row = lax.broadcasted_iota(jnp.int32, (8, TOK), 0)
        return jnp.where(row == 0, top, total)

    for i in (1, 2):

        @pl.when(z < i)
        def _():
            orecv[i - 1] = jnp.zeros_like(orecv[i - 1])
            srecv[i - 1] = jnp.broadcast_to(
                both(jnp.full((1, TOK), LOW, F32), jnp.zeros((1, TOK), F32)), (HEADS, 8, TOK)
            )

    choose()
    arrived(drow.at[1:4], R_DK)
    arrived(qrow.at[1:3], R_DQ)
    for r in range(4):
        kcol[r] = jnp.transpose(jnp.broadcast_to(drow[r][0:1, :], (128, TOK)))

    def pair(h, i, r, qd, causal=False):
        sc = dot(kvb[r, h, 0], qb[i, h], ((1,), (1,)))
        kd = kcol[r]
        mask = jnp.concatenate([kd, kd], axis=1) == qd
        if causal:
            key_at = lax.broadcasted_iota(jnp.int32, (TOK, TOK), 0)
            query_at = lax.broadcasted_iota(jnp.int32, (TOK, TOK), 1)
            mask = mask & (key_at <= query_at)
        sc = jnp.where(mask, sc, MASKED)
        top = jnp.maximum(jnp.max(sc, axis=0, keepdims=True), LOW)
        p = jnp.exp2((sc - top) * SCALE2)
        total = jnp.sum(p, axis=0, keepdims=True)
        return top, total, dot(kvb[r, h, 1], p.astype(BF), ((0,), (0,)))

    def together(results):
        top = results[0][0]
        for other, _, _ in results[1:]:
            top = jnp.maximum(top, other)
        total, acc = 0.0, 0.0
        for own, part, mixed in results:
            factor = jnp.exp2((own - top) * SCALE2)
            total = total + part * factor
            acc = acc + mixed * factor
        return top, total, acc

    def back(i, h):
        return (
            remote(
                osend.at[i - 1, h, 0:128], orecv.at[i - 1, h, 0:128], S_O, o_r.at[h],
                (((z + i) % 4) * 4 + y, m),
            ),
            remote(
                ssend.at[i - 1, h], srecv.at[i - 1, h], S_O, o_r.at[h],
                (((z + i) % 4) * 4 + y, m),
            ),
        )

    def head(h, _):
        @pl.when(h + 2 < HEADS)
        def _():
            for cp in direct(h + 2):
                cp.start()

        @pl.when(z <= 1)
        def _():
            arrived(qb.at[1:3, h], q_r.at[h])

        @pl.when(z == 2)
        def _():
            arrived(qb.at[1, h], q_r.at[h])

        q0 = qrow[0][0:1, :]
        q1 = jnp.where(z + 1 <= 3, qrow[1][0:1, :], -5.0)
        q2 = jnp.where(z + 2 <= 3, qrow[2][0:1, :], -5.0)

        def shared(n):
            if n == 0:
                return pair(h, 0, 0, q0, True)
            own = n <= y
            slot = jnp.where(own, n, jnp.where(n == y + 1, 0, n - 1))
            return pair(h, jnp.where(own, 0, 2), slot, jnp.where(own, q0, q2))

        near, mix = {}, {}
        for n in (0, 1, 3):
            near[n] = pair(h, 1, n, q1)
        mix[0] = shared(0)

        @pl.when(h + 1 < HEADS)
        def _():
            pass_on(h + 1)

        for n in (1, 4):
            mix[n] = shared(n)

        @pl.when(h == HEADS - 2)
        def _():
            for cp in wi_out:
                cp.start()

        arrived(kvb.at[2, h], kv_r.at[2, h])
        for n in (2, 3):
            mix[n] = shared(n)
        far = [
            (jnp.where(n <= y, LOW, mix[n][0]), mix[n][1], mix[n][2]) for n in (1, 2, 3)
        ] + [mix[4]]
        for i, parts_of in ((2, far), (1, None)):
            if i == 1:
                near[2] = pair(h, 1, 2, q1)
                parts_of = [near[n] for n in range(4)]
            top, total, acc = together(parts_of)
            osend[i - 1, h, 0:128] = acc.astype(BF)
            ssend[i - 1, h] = both(top, total)

            @pl.when(z + i <= 3)
            def _():
                for cp in back(i, h):
                    cp.start()

        top, total, acc = together(
            [mix[0]] + [(jnp.where(n <= y, mix[n][0], LOW), mix[n][1], mix[n][2]) for n in (1, 2, 3)]
        )
        acc0[h] = acc
        st0[h] = both(top, total)

        @pl.when(h == 0)
        def _():
            for cp in wo_loc + wo_rem:
                cp.start()

        return 0

    def pass_on(h):
        for cp in direct(h):
            cp.wait_recv()
        for cp in relay(h):
            cp.start()

    pass_on(0)
    lax.fori_loop(0, HEADS, head, 0)

    def swap(h):
        return remote(att.at[c, h], att.at[c, h], S_A, R_A, peer)

    def merge(h, _):
        @pl.when(z >= 2)
        def _():
            arrived(orecv.at[:, h], o_r.at[h])

        @pl.when(z == 1)
        def _():
            arrived(orecv.at[0, h], o_r.at[h])

        t0, t1, t2 = st0[h][0:1, :], srecv[0, h][0:1, :], srecv[1, h][0:1, :]
        n0, n1, n2 = st0[h][1:2, :], srecv[0, h][1:2, :], srecv[1, h][1:2, :]
        top = jnp.maximum(t0, jnp.maximum(t1, t2))
        f0 = jnp.exp2((t0 - top) * SCALE2)
        f1 = jnp.exp2((t1 - top) * SCALE2)
        f2 = jnp.exp2((t2 - top) * SCALE2)
        inv = 1.0 / (n0 * f0 + n1 * f1 + n2 * f2)
        mixed = (
            acc0[h] * (f0 * inv)
            + orecv[0, h, 0:128].astype(F32) * (f1 * inv)
            + orecv[1, h, 0:128].astype(F32) * (f2 * inv)
        )
        att[c, h] = jnp.transpose(mixed).astype(BF)
        swap(h).start()
        return 0

    lax.fori_loop(0, HEADS, merge, 0)

    pltpu.make_async_copy(wo.at[:, rows_c, :], wo.at[:, rows_c, :], R_WL).wait()
    arrived(wo.at[:, rows_o, :], R_WO)
    arrived(att.at[1 - c], R_A)
    both_att = jnp.concatenate([att[i, h] for i in (0, 1) for h in range(HEADS)], axis=1)

    def span(k, j):
        return slice(128 * k + 64 * j, 128 * k + 64 * j + 64)

    def project(dx, k):
        return dot(both_att[128 * k : 128 * k + 128], wo[(x + dx) % 4], ((1,), (0,)))

    def across(k):
        psend[2, 128 * k : 128 * k + 128] = project(2, k).astype(BF)
        for j, e in ((0, 1), (1, 3)):
            go(remote(psend.at[2, span(k, j)], prel.at[k, j], S_P, p_r.at[k], dev(dx=e)))

    def beside(k):
        for j, e in ((0, 1), (1, 3)):
            pnear[j, 128 * k : 128 * k + 128] = project(e, k)
            rows = span(k, 1 - j)
            psend[e, rows] = pnear[j, rows].astype(BF)
            half = slice(64 - 64 * j, 128 - 64 * j)
            go(remote(psend.at[e, rows], precv.at[k, j, half], S_P, p_r.at[2 + k], dev(dx=e)))

    def onward(k):
        arrived(prel.at[k], p_r.at[k])
        for j, e in ((0, 1), (1, 3)):
            rows = span(k, j)
            psend[e, rows] = (pnear[j, rows] + prel[k, j].astype(F32)).astype(BF)
            half = slice(64 * j, 64 * j + 64)
            go(remote(psend.at[e, rows], precv.at[k, j, half], S_P, p_r.at[2 + k], dev(dx=e)))

    across(0)
    beside(0)
    across(1)

    for j in (0, 1):
        here, cp = pass_in(j)

        @pl.when(here)
        def _():
            cp.wait_recv()
            cp.start()

    onward(0)
    beside(1)
    for k in (0, 1):
        at = slice(128 * k, 128 * k + 128)
        fown[at] = project(0, k) + res[at].astype(F32)
    onward(1)

    n_in, nd_in = {}, {}

    def tokens(r, k):
        half = slice(128 * k, 128 * k + 128)
        n_in[r, k] = go(
            remote(nb.at[0, c, half], nb.at[r, c, half], S_N, n_r.at[r - 1, k], dev(dz=r))
        )

    def mate(r, k):
        half = nb.at[r, c, 128 * k : 128 * k + 128]
        nd_in[r, k] = go(remote(half, half, S_ND, nd_r.at[r, k], peer))

    gain = gain_here[...].astype(F32).reshape(1, WID)

    def settle(k):
        at = slice(128 * k, 128 * k + 128)
        arrived(precv.at[k], p_r.at[2 + k])
        state = (fown[at] + precv[k, 0].astype(F32) + precv[k, 1].astype(F32)).astype(BF)
        res[at] = state
        nb[0, c, at] = (state.astype(F32) * gain).astype(BF)
        mate(0, k)

    settle(0)
    for r in (1, 3):
        tokens(r, 0)

    def stage_w(b):
        arrived(wou.at[0 : 2 * SLOTS], R_WU)
        for j in (0, 1):
            go(pass_out(j))

    for gi in (0, 1):
        for cs in (0, 1):
            g = 2 * c + gi
            had = jnp.logical_or(
                jnp.logical_and(g == y, c == cs), g == (left, right)[cs]
            )

            @pl.when(jnp.logical_not(had))
            def _():
                remote(hin, win_dst, wi_s.at[0], wi_r.at[gi, cs], peer).wait_recv()

    csum[...] = jnp.zeros_like(csum)
    parts = tuple(
        (r, 128 * k, 128)
        for r, k in ((0, 0), (0, 1), (1, 0), (3, 0), (2, 0), (2, 1), (1, 1), (3, 1))
    )

    plain = ()

    def quarter(b, at):
        _, first, n = parts[b]
        return pl.ds(pl.multiple_of(first + at * (n // 4), 32), n // 4)

    def eighth(b, at, j):
        _, first, n = parts[b]
        return pl.ds(pl.multiple_of(first + at * (n // 4) + j * (n // 8), 16), n // 8)

    def columns_of(r, row):
        inv_col[r] = jnp.transpose(jnp.broadcast_to(row, (128, TOK)))

    def stage_n(b):
        arrived(sqs.at[1:8], R_SQ)
        squares = sqs[0]
        for j in range(1, 8):
            squares = squares + sqs[j]
        inv_row[0] = lax.rsqrt(squares / D + EPS)
        for r in ORDER:
            go(remote(inv_row.at[0], inv_row.at[r], S_IV, R_IV, dev(dz=r)))
        columns_of(0, inv_row[0][0:1, :])

    def stage_a(b):
        r, first, n = parts[b]
        k = first // 128
        arrived(nb.at[r, c, first : first + n], n_r.at[r - 1, k])
        mate(r, k)
        if r != 2:
            half = slice(first + 32 * (r - 1), first + 32 * (r - 1) + 64)
            go(remote(nb.at[r, c, half], nb.at[2, c, half], S_N, n_r.at[1, k], dev(dz=r)))

    def stage_b(b):
        r, first, n = parts[b]
        nd_in[r, first // 128].wait_recv()
        at = slice(first, first + n)
        rows = jnp.concatenate([nb[r, 0, at], nb[r, 1, at]], axis=1)
        pre = dot(rows, win[...], ((1,), (0,)))
        prebuf[r, at] = pre
        presend[r, at] = pre.astype(BF)
        h = n // 8
        if b in plain:
            for e in (2, 1, 3):
                go(
                    remote(
                        presend.at[r, quarter(b, (x + e) % 4)], prerecv.at[b, e - 1], S_X,
                        rs_r.at[b], dev(dx=e),
                    )
                )
            return
        for j, e in ((0, 1), (1, 3)):
            rest = slice(h - j * h, 2 * h - j * h)
            go(
                remote(
                    presend.at[r, eighth(b, (x + 2) % 4, j)], relrecv.at[b, j], S_X, rel_r.at[b],
                    dev(dx=e),
                )
            )
            go(
                remote(
                    presend.at[r, eighth(b, (x + e) % 4, 1 - j)], prerecv.at[b, j, rest], S_X,
                    rs_r.at[b], dev(dx=e),
                )
            )

    def stage_r(b):
        r, first, n = parts[b]
        h = n // 8
        arrived(relrecv.at[b], rel_r.at[b])
        for j, e in ((0, 1), (1, 3)):
            half = slice(j * h, j * h + h)
            there = eighth(b, (x + e) % 4, j)
            relsend[b, j] = (
                prebuf[r, there, :] + relrecv[b, j].astype(F32)
            ).astype(BF)
            go(remote(relsend.at[b, j], prerecv.at[b, j, half], S_X, rs_r.at[b], dev(dx=e)))

    def stage_c(b):
        r, first, n = parts[b]
        arrived(prerecv.at[b, 0 : 3 if b in plain else 2], rs_r.at[b])
        if b == 2:
            arrived(inv_row.at[1:4], R_IV)
        if r and first == 0:
            columns_of(r, inv_row[r][0:1, :])
        here = quarter(b, x)
        q = slice(0, n // 4)
        pre = (
            prebuf[r, here, :] + prerecv[b, 0, q].astype(F32) + prerecv[b, 1, q].astype(F32)
        )
        if b in plain:
            pre = pre + prerecv[b, 2].astype(F32)
        factor = inv_col[r, here, :]
        active = jnp.maximum(pre, 0.0) * jnp.concatenate([factor] * 6, axis=1)
        csum[...] += jnp.sum(active, axis=0, keepdims=True)
        ab[r, c, here, :] = active.astype(BF)
        for e in (2, 1, 3) if b in plain else (1, 3):
            go(remote(ab.at[r, c, here], ab.at[r, c, here], S_X, ag_r.at[b], dev(dx=e)))

    def stage_d(b):
        r, first, n = parts[b]
        arrived(ab.at[r, c, first : first + n // 2], ag_r.at[b])
        for j, e in ((0, 1), (1, 3)):
            block = ab.at[r, c, eighth(b, (x - e) % 4, j)]
            go(remote(block, block, S_X, fwd_r.at[b], dev(dx=e)))

    def stage_g(b):
        r, first, n = parts[b]
        if b in plain:
            arrived(ab.at[r, c, first : first + 3 * n // 4], ag_r.at[b])
        else:
            arrived(ab.at[r, c, first : first + n // 4], fwd_r.at[b])
        block = ab.at[r, c, first : first + n]
        go(remote(block, block, S_AD, ad_r.at[b], peer))

    def stage_e(b):
        r, first, n = parts[b]
        if b == 0:
            arrived(wou.at[0:SLOTS], R_WP)
        arrived(ab.at[r, 1 - c, first : first + n], ad_r.at[b])
        at = slice(first, first + n)
        rows = jnp.concatenate([ab[r, 0, at], ab[r, 1, at]], axis=1)
        part = dot(rows, wou[...], ((1,), (0,)))
        if r == 0:
            fown[at] = part + res[at].astype(F32)
        else:
            k = first // 128
            for j, e in ((0, 3), (1, 1)):
                mine = slice(64 * j, 64 * j + 64)
                there = slice(first + 64 * j, first + 64 * j + 64)
                if r == 2:
                    fsend[r, there] = part[mine].astype(BF)
                    go(remote(fsend.at[r, there], frel.at[k, j], S_F, fr_r.at[k, j], dev(dz=e)))
                elif r == e:
                    fsend[r, there] = part[mine].astype(BF)
                    home(r, there)
                else:
                    fpart[k, j] = part[mine]

    def home(r, rows):
        go(remote(fsend.at[r, rows], frecv.at[r // 2, rows], S_F, R_F, dev(dz=-r)))

    def stage_q(b):
        r, first, n = parts[b]
        k, j = first // 128, r // 2
        arrived(frel.at[k, j], fr_r.at[k, j])
        rows = slice(first + 64 * j, first + 64 * j + 64)
        fsend[r, rows] = (fpart[k, j] + frel[k, j].astype(F32)).astype(BF)
        home(r, rows)

    def stage_s(b):
        for cp in wu_out:
            cp.start()
        settle(1)
        wide = res[...].astype(F32)
        square = wide * wide
        high = square.astype(BF)
        rest = (square - high.astype(F32)).astype(BF)
        ones = jnp.ones((8, WID), BF)
        sqs[0] = dot(ones, high, ((1,), (1,))) + dot(ones, rest, ((1,), (1,)))
        for j in range(1, 8):
            go(remote(sqs.at[0], sqs.at[j], S_SQ, R_SQ, dev(dx=j // 2, dc=j % 2)))

    def stage_t(b):
        tokens(parts[b][0], parts[b][1] // 128)

    def stage_h(b):
        for r in (1, 2, 3):
            go(remote(csum, csr.at[r], S_C, R_C, dev(dx=r)))

    stage = {
        "n": stage_n, "a": stage_a, "b": stage_b, "r": stage_r, "c": stage_c, "d": stage_d,
        "g": stage_g, "e": stage_e, "h": stage_h, "s": stage_s, "t": stage_t, "w": stage_w,
        "q": stage_q,
    }
    for word in PLAN:
        stage[word[0]](int(word[1]))

    arrived(csr.at[1:4], R_C)
    sums = csum[...] + csr[1] + csr[2] + csr[3]
    h_out = []
    for gi in (0, 1):
        hs[gi] = sums[:, gi * SLOTS : (gi + 1) * SLOTS]
    for gi in (0, 1):
        for cd in (0, 1):
            cp = remote(
                hs.at[gi], hsr.at[y], h_s.at[gi, cd], h_r.at[y],
                (z * 4 + 2 * c + gi, 2 * x + cd),
            )
            mine = jnp.logical_and(y == 2 * c + gi, c == cd)
            h_out.append((cp, mine))

            @pl.when(jnp.logical_not(mine))
            def _():
                cp.start()

            @pl.when(mine)
            def _():
                hsr[y] = hs[gi]

    arrived(frecv, R_F)
    out_ref[...] = (
        fown[...] + frecv[0].astype(F32) + frecv[1].astype(F32)
    ).astype(BF)

    for src in range(4):
        @pl.when(jnp.logical_not(jnp.logical_and(src == y, y // 2 == c)))
        def _():
            remote(hs.at[0], hsr.at[src], h_s.at[0, 0], h_r.at[src], peer).wait_recv()

    hm_ref[...] = (hsr[0] + hsr[1] + hsr[2] + hsr[3])[0:1, :] / TOKENS

    gone(kvb.at[0:3], S_KV)
    @pl.when(z >= 2)
    def _():
        gone(qb.at[0:2], S_Q)

    @pl.when(z == 1)
    def _():
        gone(qb.at[0], S_Q)

    @pl.when(z <= 1)
    def _():
        gone(orecv, S_O)

    @pl.when(z == 2)
    def _():
        gone(orecv.at[0], S_O)

    gone(drow.at[0:3], S_DK)
    gone(drow.at[0:2], S_DQ)
    gone(att.at[c], S_A)
    gone(wo.at[:, rows_c, :], S_WO)
    gone(psend.at[0:3], S_P)
    gone(wou.at[0 : 3 * SLOTS], S_WU)
    gone(sqs.at[1:8], S_SQ)
    gone(inv_row.at[1:4], S_IV)
    gone(fsend.at[1:4], S_N)
    gone(nb.at[0:2], S_ND)
    gone(ab.at[0:3], S_X)
    gone(presend, S_AD)
    gone(fsend.at[1:4], S_F)
    gone(csr.at[1:4], S_C)
    for cp, mine in h_out:
        @pl.when(jnp.logical_not(mine))
        def _():
            cp.wait_send()

    @pl.when(ct != c)
    def _():
        wi_peer.wait_send()

    for cp in wi_out:
        cp.wait_send()
    for j in (0, 1):
        here, cp = pass_in(j)

        @pl.when(here)
        def _():
            cp.wait_send()


def finish(layer_ref, mean_ref, out_ref, hm_ref):
    out_ref[...] = layer_ref[...]
    hm_ref[...] = mean_ref[...]


def local(resid, queries, keys, values, doc_ids, out_proj, ffn_gain, w_in, w_out, hot_index,
          hot_blocks):
    dma = pltpu.SemaphoreType.DMA
    V = pltpu.VMEM
    hbm = pl.BlockSpec(memory_space=pl.ANY)
    vm = pl.BlockSpec(memory_space=pltpu.VMEM)
    sm = pl.BlockSpec(memory_space=pltpu.SMEM)
    scratch = [
        V((1, TOK), jnp.int32), V((WID,), BF), V((1, SLOTS), jnp.int32),
        V((3, HEADS, TOK, 128), BF), V((4, HEADS, 2, TOK, 128), BF),
        V((4, 8, TOK), F32), V((3, 8, TOK), F32), V((4, TOK, 128), F32),
        V((HEADS, 128, TOK), F32), V((HEADS, 8, TOK), F32),
        V((2, HEADS, 144, TOK), BF), V((2, HEADS, 8, TOK), F32),
        V((2, HEADS, 144, TOK), BF), V((2, HEADS, 8, TOK), F32),
        V((2, HEADS, TOK, 128), BF), V((4, 2 * WID, WID), BF), V((TOK, WID), BF),
        V((4, TOK, WID), BF), V((2, 2, 128, WID), BF), V((2, 2, 64, WID), BF), V((2, TOK, WID), F32),
        V((NEUR, WID), BF), V((NEUR, WID), BF), V((WID, SLOTS), BF),
        V((2 * WID, 2 * SLOTS), BF), V((4 * SLOTS, WID), BF),
        V((8, 8, TOK), F32), V((4, 8, TOK), F32), V((4, TOK, 128), F32), V((4, 2, TOK, WID), BF),
        V((4, TOK, 2 * SLOTS), F32),
        V((4, TOK, 2 * SLOTS), BF), V((8, 3, 32, 2 * SLOTS), BF), V((8, 2, 16, 2 * SLOTS), BF),
        V((8, 2, 16, 2 * SLOTS), BF), V((4, 2, TOK, 2 * SLOTS), BF),
        V((TOK, WID), F32), V((4, TOK, WID), BF), V((2, TOK, WID), BF), V((2, 2, 64, WID), BF),
        V((2, 2, 64, WID), F32),
        V((8, 2 * SLOTS), F32), V((4, 8, 2 * SLOTS), F32), V((2, 8, SLOTS), F32),
        V((4, 8, SLOTS), F32),
        dma((17,)), dma((3, HEADS)), dma((HEADS,)), dma((HEADS,)), dma((4,)), dma((6,)), dma((2,)),
        dma((6,)), dma((2, 2)), dma((3, 2)), dma((4, 2)), dma((8,)), dma((8,)), dma((8,)),
        dma((8,)), dma((8,)), dma((2, 2)), dma((11,)), dma((2, 2)), dma((4,)),
    ]
    layer, mean = pl.pallas_call(
        kernel,
        out_shape=(
            jax.ShapeDtypeStruct((TOK, WID), BF), jax.ShapeDtypeStruct((1, SLOTS), F32),
        ),
        in_specs=[hbm] * 10 + [sm],
        out_specs=(vm, vm),
        scratch_shapes=scratch,
        compiler_params=pltpu.CompilerParams(
            collective_id=0, has_side_effects=True, vmem_limit_bytes=60 * 2**20
        ),
        name="layer",
    )(
        queries, keys, values, resid, doc_ids.reshape(1, TOK), out_proj,
        ffn_gain, w_in.T, w_out, hot_index, hot_blocks,
    )
    return pl.pallas_call(
        finish, out_shape=(
            jax.ShapeDtypeStruct((TOK, WID), BF), jax.ShapeDtypeStruct((1, SLOTS), F32),
        ), in_specs=[vm, vm], out_specs=(vm, vm), name="finish",
    )(layer, mean)


def solution(mesh):
    return jax.shard_map(
        local,
        mesh=mesh,
        in_specs=(
            P("seq", "mp"), P("seq", "mp"), P("seq", "mp"), P("seq", "mp"), P("seq"),
            P("mp", None), P("mp"), P("mp", "seq"), P("seq", "mp"), P("seq", None), P("seq"),
        ),
        out_specs=(P("seq", "mp"), P("seq", None)),
        check_vma=False,
    )
```
